128 devices in a mesh: dp: 4 (over z), row: 4 (over y), fsdp: 8 (over x, core).
Axes of the slice: x: 4, y: 4, z: 4, core: 2. Of those that a mesh axis runs over, the one named last changes fastest.
Arguments:
- x_saved: bfloat16 [2, 262144, 288], P(None, ('dp', 'row', 'fsdp'))
- dy_out: bfloat16 [2, 262144, 288], P(None, ('dp', 'row', 'fsdp'))
- w_gate: bfloat16 [288, 768], P(None, ('row', 'fsdp'))
- w_up: bfloat16 [288, 768], P(None, ('row', 'fsdp'))
- w_down: bfloat16 [768, 288], P(('row', 'fsdp'))
- g_next: float32 [128, 3, 288, 768], P(('dp', 'row', 'fsdp'))
Outputs:
- output 1: bfloat16 [2, 262144, 288], P(None, ('dp', 'row', 'fsdp'))
- output 2: float32 [3, 288, 768], P(None, None, ('row', 'fsdp'))
- output 3: float32 [128, 3, 288, 768], P(('dp', 'row', 'fsdp'))
All inputs are finite; a program needn't handle non-finite values.
Results may differ from the reference program's by a relative error of at most 0.0145274.
Values are sent between devices in bfloat16 or wider.
A program may use at most 1 GiB of HBM per device.

```python
import jax
import jax.numpy as jnp
from jax import lax

DEVICES = 128
TOK_DEV = 2048
D_MODEL = 288
FF_DIM = 768
MICRO_COUNT = 2


def setup_inputs(seed: int = 0) -> dict:
    key_list = jax.random.split(jax.random.key(seed), 6)
    tok_all = DEVICES * TOK_DEV
    act_shape = (MICRO_COUNT, tok_all, D_MODEL)
    x_saved = jax.random.normal(key_list[0], act_shape, jnp.float32)
    dy_out = jax.random.normal(key_list[1], act_shape, jnp.float32)
    w_gate = jax.random.normal(key_list[2], (D_MODEL, FF_DIM), jnp.float32) * D_MODEL ** -0.5
    w_up = jax.random.normal(key_list[3], (D_MODEL, FF_DIM), jnp.float32) * D_MODEL ** -0.5
    w_down = jax.random.normal(key_list[4], (FF_DIM, D_MODEL), jnp.float32) * FF_DIM ** -0.5
    g_next = jax.random.normal(key_list[5], (DEVICES, 3, D_MODEL, FF_DIM), jnp.float32) * DEVICES ** -0.5
    return {"x_saved": x_saved.astype(jnp.bfloat16), "dy_out": dy_out.astype(jnp.bfloat16), "w_gate": w_gate.astype(jnp.bfloat16), "w_up": w_up.astype(jnp.bfloat16), "w_down": w_down.astype(jnp.bfloat16), "g_next": g_next}


def silu_slope(pre_act):
    sigmoid_val = jax.nn.sigmoid(pre_act)
    return sigmoid_val * (1.0 + pre_act * (1.0 - sigmoid_val))


def device_backward(x_dev, dy_dev, w_gate, w_up, w_down):
    def one_micro(grad_acc, micro_pair):
        x_mb, dy_mb = micro_pair
        pre_gate = jnp.dot(x_mb, w_gate, preferred_element_type=jnp.float32)
        pre_up = jnp.dot(x_mb, w_up, preferred_element_type=jnp.float32)
        act_gate = jax.nn.silu(pre_gate)
        hidden = (act_gate * pre_up).astype(jnp.bfloat16)
        d_hidden = jnp.dot(dy_mb, w_down.T, preferred_element_type=jnp.float32)
        d_gate = (d_hidden * pre_up * silu_slope(pre_gate)).astype(jnp.bfloat16)
        d_up = (d_hidden * act_gate).astype(jnp.bfloat16)
        dx_mb = (jnp.dot(d_gate, w_gate.T, preferred_element_type=jnp.float32) + jnp.dot(d_up, w_up.T, preferred_element_type=jnp.float32)).astype(jnp.bfloat16)
        grad_mb = jnp.stack([
            jnp.dot(x_mb.T, d_gate, preferred_element_type=jnp.float32),
            jnp.dot(x_mb.T, d_up, preferred_element_type=jnp.float32),
            jnp.dot(dy_mb.T, hidden, preferred_element_type=jnp.float32),
        ])
        return grad_acc + grad_mb, dx_mb

    grad_init = jnp.zeros((3, D_MODEL, FF_DIM), jnp.float32)
    grad_sum, dx_dev = lax.scan(one_micro, grad_init, (x_dev, dy_dev))
    return dx_dev, grad_sum


def reference(x_saved, dy_out, w_gate, w_up, w_down, g_next):
    x_dev = x_saved.reshape(MICRO_COUNT, DEVICES, TOK_DEV, D_MODEL).transpose(1, 0, 2, 3)
    dy_dev = dy_out.reshape(MICRO_COUNT, DEVICES, TOK_DEV, D_MODEL).transpose(1, 0, 2, 3)

    def per_device(dev_pair):
        return device_backward(dev_pair[0], dev_pair[1], w_gate, w_up, w_down)

    dx_dev, grad_layer = lax.map(per_device, (x_dev, dy_dev))
    dx_out = dx_dev.transpose(1, 0, 2, 3).reshape(MICRO_COUNT, DEVICES * TOK_DEV, D_MODEL)
    grad_next = jnp.sum(g_next.astype(jnp.bfloat16).astype(jnp.float32), axis=0)
    return dx_out, grad_next, grad_layer
```

```python
import jax
import jax.numpy as jnp
from jax import lax
from jax.experimental import pallas as pl
from jax.experimental.pallas import tpu as pltpu
from jax.sharding import PartitionSpec as P

TOK_AXES = ("dp", "row", "fsdp")
GROUP_AXES = ("row", "fsdp")
F32, BF16 = jnp.float32, jnp.bfloat16
MESH = pl.DeviceIdType.MESH
TILE = 512
NN = (((1,), (0,)), ((), ()))
NT = (((1,), (1,)), ((), ()))


def mm(lhs, rhs, dims=NN):
    return lax.dot_general(lhs, rhs, dims, preferred_element_type=F32)


def kernel(n_dp, n_row, n_x, micro, tokens, d_model, ff, blk,
           x_hbm, dy_hbm, w1_ref, w3_ref, w2_ref, g_hbm,
           dx_hbm, gn_ref, dw_hbm,
           x_v, dy_v, dx_v, acc, g_v,
           wa, wb, w1t, w3t, w2t, w1, w3,
           gt, pr, part, rx1, up, rx2, q, ry, r, rz,
           load_sem, g_sem, out_sem, ag_s, ag_r, rs_s, rs_r):
    z, y, f = lax.axis_index("dp"), lax.axis_index("row"), lax.axis_index("fsdp")
    x, c = f // 2, f % 2
    main, tail = 256, d_model - 256

    def at_x(d):
        return (z, y, ((x + d) % n_x) * 2 + c)

    def at_y(d):
        return (z, (y + d) % n_row, f)

    def at_z(d):
        return ((z + d) % n_dp, y, f)

    partner = (z, y, x * 2 + 1 - c)
    peers = [partner] + [at_x(d) for d in range(1, n_x)] + [at_y(d) for d in range(1, n_row)]
    peers += [at_z(d) for d in range(1, n_dp)]

    barrier = pltpu.get_barrier_semaphore()
    for peer in peers:
        pl.semaphore_signal(barrier, inc=1, device_id=peer, device_id_type=MESH)

    g_loads = [pltpu.make_async_copy(g_hbm.at[s], g_v.at[s], g_sem.at[s]) for s in range(3)]
    x_load = pltpu.make_async_copy(x_hbm, x_v, load_sem.at[0])
    dy_load = pltpu.make_async_copy(dy_hbm, dy_v, load_sem.at[1])
    for load in g_loads + [x_load, dy_load]:
        load.start()

    s1, s3, s2 = w1_ref[...], w3_ref[...], w2_ref[...]
    wa[y, x, c, :, :main] = s1[:, :main]
    wa[y, x, c, :, main:] = s3[:, :main]
    wb[y, x, c, :, :main] = s2[:, :main]
    tails = [s[:, main:].astype(F32) for s in (s1, s3, s2)] + [jnp.zeros((blk, 128 - 3 * tail), F32)]
    wb[y, x, c, :, main:] = jnp.concatenate(tails, axis=1).astype(BF16)

    pl.semaphore_wait(barrier, len(peers))

    count = {"ag": 0, "rs": 0}

    def send(kind, src, dst, device):
        i = count[kind]
        count[kind] += 1
        ss, rr = (ag_s, ag_r) if kind == "ag" else (rs_s, rs_r)
        copy = pltpu.make_async_remote_copy(
            src_ref=src, dst_ref=dst, send_sem=ss.at[i], recv_sem=rr.at[i],
            device_id=device, device_id_type=MESH)
        copy.start()
        sent.append(copy)
        return copy

    sent = []

    def push(ref, device):
        return send("ag", ref, ref, device)

    a1 = [push(wa.at[y, x, c], at_x(d)) for d in (1, 3, 2)]
    b1 = [push(wb.at[y, x, c], at_y(d)) for d in (1, 3, 2)]

    def turn(s):
        g_loads[s].wait()
        flat = g_v[s, :main, :].T.reshape(n_row, n_x, 2, blk, main)
        gt[..., s * main:(s + 1) * main] = flat.astype(BF16)

    def turn_tail():
        rows = [g_v[s, main:, :] for s in range(3)] + [jnp.zeros((128 - 3 * tail, ff), F32)]
        flat = jnp.concatenate(rows, axis=0).T.reshape(n_row, n_x, 2, blk, 128)
        gt[..., 3 * main:] = flat.astype(BF16)

    turn(0)
    turn(1)

    for copy in a1:
        copy.wait_recv()
    a2 = [push(wa.at[y, :, c], at_y(1)), push(wa.at[y, :, c], at_y(n_row - 1))]
    ad = [push(wa.at[y, :, c], partner)]
    for copy in b1:
        copy.wait_recv()
    b2 = [push(wb.at[:, x, c], at_x(1)), push(wb.at[:, x, c], at_x(n_x - 1))]
    bd = [push(wb.at[:, x, c], partner)]

    turn(2)
    turn_tail()
    pair = send("rs", gt.at[:, :, 1 - c], pr, partner)

    ym, yp, yo = (y + n_row - 1) % n_row, (y + 1) % n_row, (y + 2) % n_row
    xm, xp, xo = (x + n_x - 1) % n_x, (x + 1) % n_x, (x + 2) % n_x
    a2[0].wait_recv()
    a3 = [push(wa.at[ym, pl.ds(0, 2), c], at_y(1))]
    ad.append(push(wa.at[ym, :, c], partner))
    a2[1].wait_recv()
    a3.append(push(wa.at[yp, pl.ds(2, 2), c], at_y(n_row - 1)))
    ad.append(push(wa.at[yp, :, c], partner))
    b2[0].wait_recv()
    b3 = [push(wb.at[pl.ds(0, 2), xm, c], at_x(1))]
    bd.append(push(wb.at[:, xm, c], partner))
    b2[1].wait_recv()
    b3.append(push(wb.at[pl.ds(2, 2), xp, c], at_x(n_x - 1)))
    bd.append(push(wb.at[:, xp, c], partner))

    pair.wait_recv()
    part[...] = (gt[:, :, c].astype(F32) + pr[...].astype(F32)).astype(BF16)
    hy = n_row // 2

    for copy in a3:
        copy.wait_recv()
    ad.append(push(wa.at[yo, :, c], partner))
    for copy in b3:
        copy.wait_recv()
    bd.append(push(wb.at[:, xo, c], partner))

    x1 = [send("rs", part.at[pl.ds(0, hy), xo], rx1.at[0], at_x(1)),
          send("rs", part.at[pl.ds(hy, hy), xo], rx1.at[1], at_x(n_x - 1))]

    acc[...] = jnp.zeros_like(acc)
    for copy in ad + bd:
        copy.wait_recv()

    def flat(ref, lo, hi):
        return ref[..., lo:hi].astype(F32).reshape(ff, hi - lo).astype(BF16)

    m1, m3, m2, mt = flat(wa, 0, main), flat(wa, main, 2 * main), flat(wb, 0, main), flat(wb, main, main + 128)
    w1t[:, :main] = m1
    w3t[:, :main] = m3
    w2t[:, :main] = m2
    w1t[:, main:] = mt[:, :tail]
    w3t[:, main:] = mt[:, tail:2 * tail]
    w2t[:, main:] = mt[:, 2 * tail:3 * tail]
    w1[:main, :] = m1.T
    w3[:main, :] = m3.T
    tail_t = mt.T
    w1[main:, :] = tail_t[:tail]
    w3[main:, :] = tail_t[tail:2 * tail]
    x_load.wait()
    dy_load.wait()

    per = tokens // TILE
    steps = micro * per

    def stage_up():
        for copy in x1:
            copy.wait_recv()
        up[0, hy:] = part[hy:, xp]
        up[0, :hy] = (part[:hy, xp].astype(F32) + rx1[0].astype(F32)).astype(BF16)
        up[1, :hy] = part[:hy, xm]
        up[1, hy:] = (part[hy:, xm].astype(F32) + rx1[1].astype(F32)).astype(BF16)

    def out_copy(i):
        m, t = i // per, i % per
        where = pl.ds(pl.multiple_of(t * TILE, TILE), TILE)
        return pltpu.make_async_copy(dx_v.at[m, :, where], dx_hbm.at[m, :, where], out_sem.at[i])

    def step(i, carry):
        m, t = i // per, i % per
        where = pl.ds(pl.multiple_of(t * TILE, TILE), TILE)
        xt, dyt = x_v[m, :, where], dy_v[m, :, where]
        a, b, dh = mm(w1t[...], xt), mm(w3t[...], xt), mm(w2t[...], dyt)
        sig = 0.5 * jnp.tanh(0.5 * a) + 0.5
        act = a * sig
        h = (act * b).astype(BF16)
        db = (dh * act).astype(BF16)
        da = (dh * b * (sig + act * (1.0 - sig))).astype(BF16)
        dx_v[m, :, where] = (mm(w1[...], da) + mm(w3[...], db)).astype(BF16)
        acc[0] += mm(xt, da, NT)
        acc[1] += mm(xt, db, NT)
        acc[2] += mm(dyt, h, NT)
        out_copy(i).start()
        return carry

    quarter = steps // 4
    lax.fori_loop(0, quarter, step, 0)
    stage_up()
    x2 = [send("rs", up.at[0], rx2.at[0], at_x(1)), send("rs", up.at[1], rx2.at[1], at_x(n_x - 1))]
    lax.fori_loop(quarter, 2 * quarter, step, 0)
    for copy in x2:
        copy.wait_recv()
    q[...] = (part[:, x].astype(F32) + rx2[0].astype(F32) + rx2[1].astype(F32)).astype(BF16)
    ys = [send("rs", q.at[(y + d) % n_row], ry.at[d - 1], at_y(d)) for d in range(1, n_row)]
    lax.fori_loop(2 * quarter, 3 * quarter, step, 0)
    for copy in ys:
        copy.wait_recv()
    own = q[y].astype(F32)
    for d in range(1, n_row):
        own += ry[d - 1].astype(F32)
    r[...] = own.astype(BF16)
    zs = [send("rs", r, rz.at[z], at_z(d)) for d in range(1, n_dp)]
    rz[z] = r[...]
    lax.fori_loop(3 * quarter, steps, step, 0)
    dw_out = [pltpu.make_async_copy(acc.at[s], dw_hbm.at[s], g_sem.at[s]) for s in range(3)]
    for copy in dw_out:
        copy.start()
    for copy in zs:
        copy.wait_recv()
    total = rz[0].astype(F32)
    for d in range(1, n_dp):
        total += rz[d].astype(F32)
    for s in range(3):
        gn_ref[s, :, :main] = total[:, s * main:(s + 1) * main]
        gn_ref[s, :, main:] = total[:, 3 * main + s * tail:3 * main + (s + 1) * tail]
    for copy in sent:
        copy.wait_send()
    for copy in dw_out:
        copy.wait()
    for i in range(steps):
        out_copy(i).wait()


def solution(mesh):
    n_dp, n_row, n_x = mesh.shape["dp"], mesh.shape["row"], mesh.shape["fsdp"] // 2

    def local_step(x_dev, dy_dev, gate, up_w, down, g_dev):
        micro, tokens, d_model = x_dev.shape
        blk = gate.shape[1]
        ff = blk * n_row * n_x * 2
        wide = 3 * 256 + 128
        vmem = pl.BlockSpec(memory_space=pltpu.VMEM)
        hbm = pl.BlockSpec(memory_space=pltpu.HBM)

        def body(*refs):
            kernel(n_dp, n_row, n_x, micro, tokens, d_model, ff, blk, *refs)

        steps = micro * (tokens // TILE)
        dx_t, gn, dw = pl.pallas_call(
            body,
            in_specs=[hbm, hbm, vmem, vmem, vmem, hbm],
            out_specs=[hbm, vmem, hbm],
            out_shape=[
                jax.ShapeDtypeStruct((micro, d_model, tokens), BF16),
                jax.ShapeDtypeStruct((3, blk, d_model), F32),
                jax.ShapeDtypeStruct((3, d_model, ff), F32),
            ],
            scratch_shapes=[
                pltpu.VMEM((micro, d_model, tokens), BF16),
                pltpu.VMEM((micro, d_model, tokens), BF16),
                pltpu.VMEM((micro, d_model, tokens), BF16),
                pltpu.VMEM((3, d_model, ff), F32),
                pltpu.VMEM((3, d_model, ff), F32),
                pltpu.VMEM((n_row, n_x, 2, blk, 512), BF16),
                pltpu.VMEM((n_row, n_x, 2, blk, 384), BF16),
                pltpu.VMEM((ff, d_model), BF16),
                pltpu.VMEM((ff, d_model), BF16),
                pltpu.VMEM((ff, d_model), BF16),
                pltpu.VMEM((d_model, ff), BF16),
                pltpu.VMEM((d_model, ff), BF16),
                pltpu.VMEM((n_row, n_x, 2, blk, wide), BF16),
                pltpu.VMEM((n_row, n_x, blk, wide), BF16),
                pltpu.VMEM((n_row, n_x, blk, wide), BF16),
                pltpu.VMEM((2, n_row // 2, blk, wide), BF16),
                pltpu.VMEM((2, n_row, blk, wide), BF16),
                pltpu.VMEM((2, n_row, blk, wide), BF16),
                pltpu.VMEM((n_row, blk, wide), BF16),
                pltpu.VMEM((n_row - 1, blk, wide), BF16),
                pltpu.VMEM((blk, wide), BF16),
                pltpu.VMEM((n_dp, blk, wide), BF16),
                pltpu.SemaphoreType.DMA((2,)),
                pltpu.SemaphoreType.DMA((3,)),
                pltpu.SemaphoreType.DMA((steps,)),
                pltpu.SemaphoreType.DMA((22,)),
                pltpu.SemaphoreType.DMA((22,)),
                pltpu.SemaphoreType.DMA((11,)),
                pltpu.SemaphoreType.DMA((11,)),
            ],
            compiler_params=pltpu.CompilerParams(
                collective_id=0, has_side_effects=True, vmem_limit_bytes=60 * 2**20),
            name="mlp_step",
        )(x_dev.transpose(0, 2, 1), dy_dev.transpose(0, 2, 1), gate.T, up_w.T, down, g_dev[0])
        return dx_t.transpose(0, 2, 1), gn.transpose(0, 2, 1), dw[None]

    in_specs = (P(None, TOK_AXES, None), P(None, TOK_AXES, None), P(None, GROUP_AXES), P(None, GROUP_AXES), P(GROUP_AXES, None), P(TOK_AXES, None, None, None))
    out_specs = (P(None, TOK_AXES, None), P(None, None, GROUP_AXES), P(TOK_AXES, None, None, None))
    return jax.shard_map(local_step, mesh=mesh, in_specs=in_specs, out_specs=out_specs, check_vma=False)
```

```python
import jax
import jax.numpy as jnp
from jax import lax
from jax.experimental import pallas as pl
from jax.experimental.pallas import tpu as pltpu
from jax.sharding import PartitionSpec as P

TOK_AXES = ("dp", "row", "fsdp")
GROUP_AXES = ("row", "fsdp")
F32, BF16 = jnp.float32, jnp.bfloat16
MESH = pl.DeviceIdType.MESH
TILE = 512
NN = (((1,), (0,)), ((), ()))
NT = (((1,), (1,)), ((), ()))


def mm(lhs, rhs, dims=NN):
    return lax.dot_general(lhs, rhs, dims, preferred_element_type=F32)


def kernel(n_dp, n_row, n_x, micro, tokens, d_model, ff, blk,
           x_hbm, dy_hbm, w1_hbm, w3_hbm, w2_hbm, g_hbm,
           dx_v, gn_ref, acc,
           x_v, dy_v, g_v, shard,
           wa, wb, w1t, w3t, w2t, w1, w3,
           gt, pr, part, rx1, up, rx2, q, ry, r, rz,
           load_sem, g_sem, ag_s, ag_r, rs_s, rs_r):
    z, y, f = lax.axis_index("dp"), lax.axis_index("row"), lax.axis_index("fsdp")
    x, c = f // 2, f % 2
    main, tail = 256, d_model - 256

    def at_x(d):
        return (z, y, ((x + d) % n_x) * 2 + c)

    def at_y(d):
        return (z, (y + d) % n_row, f)

    def at_z(d):
        return ((z + d) % n_dp, y, f)

    partner = (z, y, x * 2 + 1 - c)
    peers = [partner] + [at_x(d) for d in range(1, n_x)] + [at_y(d) for d in range(1, n_row)]
    peers += [at_z(d) for d in range(1, n_dp)]

    barrier = pltpu.get_barrier_semaphore()
    for peer in peers:
        pl.semaphore_signal(barrier, inc=1, device_id=peer, device_id_type=MESH)

    g_loads = [pltpu.make_async_copy(g_hbm.at[s], g_v.at[s], g_sem.at[s]) for s in range(3)]
    x_load = pltpu.make_async_copy(x_hbm, x_v, load_sem.at[0])
    dy_load = pltpu.make_async_copy(dy_hbm, dy_v, load_sem.at[1])
    w_loads = [pltpu.make_async_copy(w, shard.at[i], load_sem.at[2 + i]) for i, w in enumerate((w1_hbm, w3_hbm, w2_hbm))]
    for load in w_loads + g_loads + [x_load, dy_load]:
        load.start()
    for load in w_loads:
        load.wait()

    s1, s3, s2 = shard[0], shard[1], shard[2]
    wa[y, x, c, :, :main] = s1[:, :main]
    wa[y, x, c, :, main:] = s3[:, :main]
    wb[y, x, c, :, :main] = s2[:, :main]
    tails = [s[:, main:].astype(F32) for s in (s1, s3, s2)] + [jnp.zeros((blk, 128 - 3 * tail), F32)]
    wb[y, x, c, :, main:] = jnp.concatenate(tails, axis=1).astype(BF16)

    pl.semaphore_wait(barrier, len(peers))

    count = {"ag": 0, "rs": 0}

    def send(kind, src, dst, device):
        i = count[kind]
        count[kind] += 1
        ss, rr = (ag_s, ag_r) if kind == "ag" else (rs_s, rs_r)
        copy = pltpu.make_async_remote_copy(
            src_ref=src, dst_ref=dst, send_sem=ss.at[i], recv_sem=rr.at[i],
            device_id=device, device_id_type=MESH)
        copy.start()
        sent.append(copy)
        return copy

    sent = []

    def push(ref, device):
        return send("ag", ref, ref, device)

    a1 = [push(wa.at[y, x, c], at_x(d)) for d in (1, 3, 2)]
    b1 = [push(wb.at[y, x, c], at_y(d)) for d in (1, 3, 2)]

    def turn(s):
        g_loads[s].wait()
        flat = g_v[s, :main, :].T.reshape(n_row, n_x, 2, blk, main)
        gt[..., s * main:(s + 1) * main] = flat.astype(BF16)

    def turn_tail():
        rows = [g_v[s, main:, :] for s in range(3)] + [jnp.zeros((128 - 3 * tail, ff), F32)]
        flat = jnp.concatenate(rows, axis=0).T.reshape(n_row, n_x, 2, blk, 128)
        gt[..., 3 * main:] = flat.astype(BF16)

    turn(0)
    turn(1)

    for copy in a1:
        copy.wait_recv()
    a2 = [push(wa.at[y, :, c], at_y(1)), push(wa.at[y, :, c], at_y(n_row - 1))]
    ad = [push(wa.at[y, :, c], partner)]
    for copy in b1:
        copy.wait_recv()
    b2 = [push(wb.at[:, x, c], at_x(1)), push(wb.at[:, x, c], at_x(n_x - 1))]
    bd = [push(wb.at[:, x, c], partner)]

    turn(2)
    turn_tail()
    pair = send("rs", gt.at[:, :, 1 - c], pr, partner)

    ym, yp, yo = (y + n_row - 1) % n_row, (y + 1) % n_row, (y + 2) % n_row
    xm, xp, xo = (x + n_x - 1) % n_x, (x + 1) % n_x, (x + 2) % n_x
    a2[0].wait_recv()
    a3 = [push(wa.at[ym, pl.ds(0, 2), c], at_y(1))]
    ad.append(push(wa.at[ym, :, c], partner))
    a2[1].wait_recv()
    a3.append(push(wa.at[yp, pl.ds(2, 2), c], at_y(n_row - 1)))
    ad.append(push(wa.at[yp, :, c], partner))
    b2[0].wait_recv()
    b3 = [push(wb.at[pl.ds(0, 2), xm, c], at_x(1))]
    bd.append(push(wb.at[:, xm, c], partner))
    b2[1].wait_recv()
    b3.append(push(wb.at[pl.ds(2, 2), xp, c], at_x(n_x - 1)))
    bd.append(push(wb.at[:, xp, c], partner))

    pair.wait_recv()
    part[...] = (gt[:, :, c].astype(F32) + pr[...].astype(F32)).astype(BF16)
    hy = n_row // 2

    for copy in a3:
        copy.wait_recv()
    ad.append(push(wa.at[yo, :, c], partner))
    for copy in b3:
        copy.wait_recv()
    bd.append(push(wb.at[:, xo, c], partner))

    x1 = [send("rs", part.at[pl.ds(0, hy), xo], rx1.at[0], at_x(1)),
          send("rs", part.at[pl.ds(hy, hy), xo], rx1.at[1], at_x(n_x - 1))]

    acc[...] = jnp.zeros_like(acc)
    for copy in ad + bd:
        copy.wait_recv()

    def flat(ref, lo, hi):
        return ref[..., lo:hi].astype(F32).reshape(ff, hi - lo).astype(BF16)

    m1, m3, m2, mt = flat(wa, 0, main), flat(wa, main, 2 * main), flat(wb, 0, main), flat(wb, main, main + 128)
    w1t[:, :main] = m1
    w3t[:, :main] = m3
    w2t[:, :main] = m2
    w1t[:, main:] = mt[:, :tail]
    w3t[:, main:] = mt[:, tail:2 * tail]
    w2t[:, main:] = mt[:, 2 * tail:3 * tail]
    w1[:main, :] = m1.T
    w3[:main, :] = m3.T
    tail_t = mt.T
    w1[main:, :] = tail_t[:tail]
    w3[main:, :] = tail_t[tail:2 * tail]
    x_load.wait()
    dy_load.wait()

    per = tokens // TILE
    steps = micro * per

    def stage_up():
        for copy in x1:
            copy.wait_recv()
        up[0, hy:] = part[hy:, xp]
        up[0, :hy] = (part[:hy, xp].astype(F32) + rx1[0].astype(F32)).astype(BF16)
        up[1, :hy] = part[:hy, xm]
        up[1, hy:] = (part[hy:, xm].astype(F32) + rx1[1].astype(F32)).astype(BF16)

    def step(i, carry):
        m, t = i // per, i % per
        where = pl.ds(pl.multiple_of(t * TILE, TILE), TILE)
        xt, dyt = x_v[m, :, where], dy_v[m, :, where]
        a, b, dh = mm(w1t[...], xt), mm(w3t[...], xt), mm(w2t[...], dyt)
        sig = 0.5 * jnp.tanh(0.5 * a) + 0.5
        act = a * sig
        h = (act * b).astype(BF16)
        db = (dh * act).astype(BF16)
        da = (dh * b * (sig + act * (1.0 - sig))).astype(BF16)
        dx_v[m, :, where] = (mm(w1[...], da) + mm(w3[...], db)).astype(BF16)
        acc[0] += mm(xt, da, NT)
        acc[1] += mm(xt, db, NT)
        acc[2] += mm(dyt, h, NT)
        return carry

    quarter = steps // 4
    lax.fori_loop(0, quarter, step, 0)
    stage_up()
    x2 = [send("rs", up.at[0], rx2.at[0], at_x(1)), send("rs", up.at[1], rx2.at[1], at_x(n_x - 1))]
    lax.fori_loop(quarter, 2 * quarter, step, 0)
    for copy in x2:
        copy.wait_recv()
    q[...] = (part[:, x].astype(F32) + rx2[0].astype(F32) + rx2[1].astype(F32)).astype(BF16)
    ys = [send("rs", q.at[(y + d) % n_row], ry.at[d - 1], at_y(d)) for d in range(1, n_row)]
    lax.fori_loop(2 * quarter, 3 * quarter, step, 0)
    for copy in ys:
        copy.wait_recv()
    own = q[y].astype(F32)
    for d in range(1, n_row):
        own += ry[d - 1].astype(F32)
    r[...] = own.astype(BF16)
    zs = [send("rs", r, rz.at[z], at_z(d)) for d in range(1, n_dp)]
    rz[z] = r[...]
    lax.fori_loop(3 * quarter, steps, step, 0)
    for copy in zs:
        copy.wait_recv()
    total = rz[0].astype(F32)
    for d in range(1, n_dp):
        total += rz[d].astype(F32)
    for s in range(3):
        gn_ref[s, :, :main] = total[:, s * main:(s + 1) * main]
        gn_ref[s, :, main:] = total[:, 3 * main + s * tail:3 * main + (s + 1) * tail]
    for copy in sent:
        copy.wait_send()


def write_out(*refs):
    n = len(refs) // 2
    sems = refs[-1]
    copies = [pltpu.make_async_copy(refs[i], refs[n + i], sems.at[i]) for i in range(n)]
    for copy in copies:
        copy.start()
    for copy in copies:
        copy.wait()


def solution(mesh):
    n_dp, n_row, n_x = mesh.shape["dp"], mesh.shape["row"], mesh.shape["fsdp"] // 2

    def local_step(x_dev, dy_dev, gate, up_w, down, g_dev):
        micro, tokens, d_model = x_dev.shape
        blk = gate.shape[1]
        ff = blk * n_row * n_x * 2
        wide = 3 * 256 + 128
        vmem = pl.BlockSpec(memory_space=pltpu.VMEM)
        hbm = pl.BlockSpec(memory_space=pltpu.HBM)

        def body(*refs):
            kernel(n_dp, n_row, n_x, micro, tokens, d_model, ff, blk, *refs)

        shapes = [((micro, d_model, tokens), BF16), ((3, blk, d_model), F32), ((3, d_model, ff), F32)]
        args = [x_dev.transpose(0, 2, 1), dy_dev.transpose(0, 2, 1), gate.T, up_w.T, down, g_dev[0]]
        args = [pltpu.with_memory_space_constraint(arg, pltpu.HBM) for arg in args]
        parts = pl.pallas_call(
            body,
            in_specs=[hbm] * 6,
            out_specs=[vmem] * 3,
            out_shape=[pltpu.VMEM(*shape) for shape in shapes],
            scratch_shapes=[
                pltpu.VMEM((micro, d_model, tokens), BF16),
                pltpu.VMEM((micro, d_model, tokens), BF16),
                pltpu.VMEM((3, d_model, ff), F32),
                pltpu.VMEM((3, blk, d_model), BF16),
                pltpu.VMEM((n_row, n_x, 2, blk, 512), BF16),
                pltpu.VMEM((n_row, n_x, 2, blk, 384), BF16),
                pltpu.VMEM((ff, d_model), BF16),
                pltpu.VMEM((ff, d_model), BF16),
                pltpu.VMEM((ff, d_model), BF16),
                pltpu.VMEM((d_model, ff), BF16),
                pltpu.VMEM((d_model, ff), BF16),
                pltpu.VMEM((n_row, n_x, 2, blk, wide), BF16),
                pltpu.VMEM((n_row, n_x, blk, wide), BF16),
                pltpu.VMEM((n_row, n_x, blk, wide), BF16),
                pltpu.VMEM((2, n_row // 2, blk, wide), BF16),
                pltpu.VMEM((2, n_row, blk, wide), BF16),
                pltpu.VMEM((2, n_row, blk, wide), BF16),
                pltpu.VMEM((n_row, blk, wide), BF16),
                pltpu.VMEM((n_row - 1, blk, wide), BF16),
                pltpu.VMEM((blk, wide), BF16),
                pltpu.VMEM((n_dp, blk, wide), BF16),
                pltpu.SemaphoreType.DMA((5,)),
                pltpu.SemaphoreType.DMA((3,)),
                pltpu.SemaphoreType.DMA((22,)),
                pltpu.SemaphoreType.DMA((22,)),
                pltpu.SemaphoreType.DMA((11,)),
                pltpu.SemaphoreType.DMA((11,)),
            ],
            compiler_params=pltpu.CompilerParams(
                collective_id=0, has_side_effects=True, vmem_limit_bytes=44 * 2**20),
            name="mlp_step",
        )(*args)
        dx_t, gn, dw = pl.pallas_call(
            write_out,
            in_specs=[vmem] * 3,
            out_specs=[hbm] * 3,
            out_shape=[jax.ShapeDtypeStruct(*shape) for shape in shapes],
            scratch_shapes=[pltpu.SemaphoreType.DMA((3,))],
            compiler_params=pltpu.CompilerParams(vmem_limit_bytes=2 * 2**20),
            name="write_out",
        )(*parts)
        return dx_t.transpose(0, 2, 1), gn.transpose(0, 2, 1), dw[None]

    in_specs = (P(None, TOK_AXES, None), P(None, TOK_AXES, None), P(None, GROUP_AXES), P(None, GROUP_AXES), P(GROUP_AXES, None), P(TOK_AXES, None, None, None))
    out_specs = (P(None, TOK_AXES, None), P(None, None, GROUP_AXES), P(TOK_AXES, None, None, None))
    return jax.shard_map(local_step, mesh=mesh, in_specs=in_specs, out_specs=out_specs, check_vma=False)
```

```python
import jax
import jax.numpy as jnp
from jax import lax
from jax.experimental import pallas as pl
from jax.experimental.pallas import tpu as pltpu
from jax.sharding import PartitionSpec as P

TOK_AXES = ("dp", "row", "fsdp")
GROUP_AXES = ("row", "fsdp")
F32, BF16 = jnp.float32, jnp.bfloat16
MESH = pl.DeviceIdType.MESH
NN = (((1,), (0,)), ((), ()))
NT = (((1,), (1,)), ((), ()))


def mm(lhs, rhs, dims=NN):
    return lax.dot_general(lhs, rhs, dims, preferred_element_type=F32)


def kernel(n_dp, n_row, n_x, micro, tokens, d_model, ff, blk,
           x_hbm, dy_hbm, w1_hbm, w3_hbm, w2_hbm, g_hbm,
           dx_v, gn_ref, acc,
           x_v, dy_v, g_v, shard, wbuf, g1, g3, g2, w1, w3, hs, das, dbs,
           gt, pr, part, rx1, rx0, mid, rx2, q, ry, r, rz,
           load_sem, g_sem, ag_s, ag_r, rs_s, rs_r):
    z, y, f = lax.axis_index("dp"), lax.axis_index("row"), lax.axis_index("fsdp")
    x, c = f // 2, f % 2
    main, tail = 256, d_model - 256
    side = n_x
    rows = 2 * blk

    def chip(du, dv):
        return (y + dv * (1 - c) + du * c + side) % side, (x + du * (1 - c) + dv * c + side) % side

    def device(du, dv):
        yy, xx = chip(du, dv)
        return (z, yy, xx * 2 + c)

    def at_z(d):
        return ((z + d) % n_dp, y, f)

    partner = (z, y, x * 2 + 1 - c)
    peers = [partner, device(1, 0), device(-1, 0), device(0, 1), device(0, -1), device(0, 2)]
    peers += [at_z(d) for d in range(1, n_dp)]

    barrier = pltpu.get_barrier_semaphore()
    for peer in peers:
        pl.semaphore_signal(barrier, inc=1, device_id=peer, device_id_type=MESH)

    g_loads = [pltpu.make_async_copy(g_hbm.at[s], g_v.at[s], g_sem.at[s]) for s in range(3)]
    x_load = pltpu.make_async_copy(x_hbm, x_v, load_sem.at[0])
    dy_load = pltpu.make_async_copy(dy_hbm, dy_v, load_sem.at[1])
    w_loads = [pltpu.make_async_copy(w, shard.at[i], load_sem.at[2 + i]) for i, w in enumerate((w1_hbm, w3_hbm, w2_hbm))]
    for load in w_loads + g_loads + [x_load, dy_load]:
        load.start()
    for load in w_loads:
        load.wait()

    s1, s3, s2 = shard[0], shard[1], shard[2]
    wbuf[y, x, c, :, :main] = s1[:, :main]
    wbuf[y, x, c, :, main:2 * main] = s3[:, :main]
    wbuf[y, x, c, :, 2 * main:3 * main] = s2[:, :main]
    tails = [s[:, main:].astype(F32) for s in (s1, s3, s2)] + [jnp.zeros((blk, 128 - 3 * tail), F32)]
    wbuf[y, x, c, :, 3 * main:] = jnp.concatenate(tails, axis=1).astype(BF16)

    pl.semaphore_wait(barrier, len(peers))

    sent = []
    count = {"ag": 0, "rs": 0}

    def send(kind, src, dst, where):
        i = count[kind]
        count[kind] += 1
        ss, rr = (ag_s, ag_r) if kind == "ag" else (rs_s, rs_r)
        copy = pltpu.make_async_remote_copy(
            src_ref=src, dst_ref=dst, send_sem=ss.at[i], recv_sem=rr.at[i],
            device_id=where, device_id_type=MESH)
        copy.start()
        sent.append(copy)
        return copy

    arrive, pairs = {}, {}

    def forward(du, dv, su, sv):
        ref = wbuf.at[(*chip(du, dv), c)]
        got = tuple((a - b + 1) % side - 1 for a, b in ((du, su), (dv, sv)))
        arrive[got] = send("ag", ref, ref, device(su, sv))

    def share(du, dv):
        ref = wbuf.at[(*chip(du, dv), c)]
        pairs[du, dv] = send("ag", ref, ref, partner)

    def take(du, dv, *steps):
        arrive[du, dv].wait_recv()
        for su, sv in steps:
            forward(du, dv, su, sv)
        share(du, dv)

    for su, sv in ((1, 0), (-1, 0), (0, 1), (0, -1)):
        forward(0, 0, su, sv)
    share(0, 0)

    def turn(s):
        g_loads[s].wait()
        flat = g_v[s, :main, :].T.reshape(n_row, n_x, 2, blk, main)
        gt[..., s * main:(s + 1) * main] = flat.astype(BF16)

    def turn_tail():
        parts = [g_v[s, main:, :] for s in range(3)] + [jnp.zeros((128 - 3 * tail, ff), F32)]
        flat = jnp.concatenate(parts, axis=0).T.reshape(n_row, n_x, 2, blk, 128)
        gt[..., 3 * main:] = flat.astype(BF16)

    def fill(group):
        for j, (du, dv) in enumerate(group):
            both = wbuf[chip(du, dv)].astype(F32).reshape(rows, 3 * main + 128).astype(BF16)
            at = slice(j * rows, (j + 1) * rows)
            for i, ref in enumerate((g1, g3, g2)):
                ref[at, :main] = both[:, i * main:(i + 1) * main]
                ref[at, main:] = both[:, 3 * main + i * tail:3 * main + (i + 1) * tail]

    def ahead(group, m):
        n = len(group) * rows
        to = pl.ds(pl.multiple_of(m * tokens, tokens), tokens)
        xt, dyt = x_v[m], dy_v[m]
        a, b, dh = mm(g1[:n], xt), mm(g3[:n], xt), mm(g2[:n], dyt)
        sig = 0.5 * jnp.tanh(0.5 * a) + 0.5
        act = a * sig
        h = (act * b).astype(BF16)
        db = (dh * act).astype(BF16)
        da = (dh * b * (sig + act * (1.0 - sig))).astype(BF16)
        for j, (du, dv) in enumerate(group):
            yy, xx = chip(du, dv)
            first = pl.multiple_of((yy * n_x + xx) * rows, 16)
            at = slice(j * rows, (j + 1) * rows)
            hs[pl.ds(first, rows), to] = h[at]
            das[pl.ds(first, rows), to] = da[at]
            dbs[pl.ds(first, rows), to] = db[at]

    def back(m):
        to = pl.ds(pl.multiple_of(m * tokens, tokens), tokens)
        xt, dyt = x_v[m], dy_v[m]
        h, da, db = hs[:, to], das[:, to], dbs[:, to]
        dx_v[m] = (mm(w1[...], da) + mm(w3[...], db)).astype(BF16)
        acc[0] += mm(xt, da, NT)
        acc[1] += mm(xt, db, NT)
        acc[2] += mm(dyt, h, NT)

    turn(0)
    turn(1)
    turn(2)
    turn_tail()
    pair = send("rs", gt.at[:, :, 1 - c], pr, partner)
    acc[...] = jnp.zeros_like(acc)
    x_load.wait()
    dy_load.wait()
    pairs[0, 0].wait_recv()
    fill([(0, 0)])
    ahead([(0, 0)], 0)

    take(-1, 0, (1, 0), (0, 1), (0, -1))
    take(1, 0, (0, 1), (0, -1))
    take(0, -1, (0, 1))
    take(0, 1)
    pair.wait_recv()
    for yy in range(n_row):
        for xx in range(n_x):
            both = gt[yy, xx, c].astype(F32) + pr[yy, xx].astype(F32)
            part[xx * (1 - c) + yy * c, yy * (1 - c) + xx * c] = both.astype(BF16)
    u, v = x * (1 - c) + y * c, y * (1 - c) + x * c
    um, up, uo = (u + side - 1) % side, (u + 1) % side, (u + 2) % side
    lo, hi = pl.ds(0, side // 2), pl.ds(side // 2, side // 2)

    u1 = [send("rs", part.at[uo, lo], rx1.at[0], device(1, 0)),
          send("rs", part.at[uo, hi], rx1.at[1], device(-1, 0))]
    u0 = [send("rs", part.at[up, hi], rx0.at[0], device(1, 0)),
          send("rs", part.at[um, lo], rx0.at[1], device(-1, 0))]
    ahead([(0, 0)], 1)
    near = [(-1, 0), (1, 0), (0, -1), (0, 1)]
    for key in near:
        pairs[key].wait_recv()
    fill(near)
    ahead(near, 0)
    take(2, 0, (0, 1), (0, -1))
    take(-1, -1, (0, 1))
    take(1, 1, (0, -1))
    take(-1, 1)
    take(1, -1)
    take(0, 2)
    ahead(near, 1)
    mids = [(2, 0), (0, 2), (-1, -1), (1, 1), (-1, 1), (1, -1)]
    for key in mids:
        pairs[key].wait_recv()
    fill(mids)
    ahead(mids, 0)
    take(2, 1, (0, -1))
    take(2, -1)
    take(-1, 2)
    take(1, 2)
    ahead(mids, 1)

    for copy in u1:
        copy.wait_recv()
    half = side // 2
    mid[0] = (part[up, :half].astype(F32) + rx1[0].astype(F32)).astype(BF16)
    mid[1] = (part[um, half:].astype(F32) + rx1[1].astype(F32)).astype(BF16)
    u2 = [send("rs", mid.at[0], rx2.at[0], device(1, 0)), send("rs", mid.at[1], rx2.at[1], device(-1, 0))]

    far = [(2, 1), (2, -1), (-1, 2), (1, 2)]
    for key in far:
        pairs[key].wait_recv()
    fill(far)
    ahead(far, 0)
    take(2, 2)
    ahead(far, 1)
    pairs[2, 2].wait_recv()
    fill([(2, 2)])

    for copy in u0 + u2:
        copy.wait_recv()
    q[:half] = (part[u, :half].astype(F32) + rx2[0].astype(F32) + rx0[1].astype(F32)).astype(BF16)
    q[half:] = (part[u, half:].astype(F32) + rx2[1].astype(F32) + rx0[0].astype(F32)).astype(BF16)
    vs = [send("rs", q.at[(v + d) % side], ry.at[d - 1], device(0, d)) for d in (2, 1, 3)]

    def across(lo, hi):
        return wbuf[..., lo:hi].astype(F32).reshape(ff, hi - lo).astype(BF16).T

    w1[:main, :] = across(0, main)
    w3[:main, :] = across(main, 2 * main)
    ends = across(3 * main, 3 * main + 128)
    w1[main:, :] = ends[:tail]
    w3[main:, :] = ends[tail:2 * tail]

    ahead([(2, 2)], 0)
    back(0)
    for copy in vs:
        copy.wait_recv()
    own = q[v].astype(F32)
    for d in range(1, side):
        own += ry[d - 1].astype(F32)
    r[...] = own.astype(BF16)
    zs = [send("rs", r, rz.at[z], at_z(d)) for d in (2, 1, 3)]
    rz[z] = r[...]
    ahead([(2, 2)], 1)
    back(1)
    for copy in zs:
        copy.wait_recv()
    total = rz[0].astype(F32)
    for d in range(1, n_dp):
        total += rz[d].astype(F32)
    for s in range(3):
        gn_ref[s, :, :main] = total[:, s * main:(s + 1) * main]
        gn_ref[s, :, main:] = total[:, 3 * main + s * tail:3 * main + (s + 1) * tail]
    for copy in sent:
        copy.wait_send()


def write_out(*refs):
    n = len(refs) // 2
    sems = refs[-1]
    copies = [pltpu.make_async_copy(refs[i], refs[n + i], sems.at[i]) for i in range(n)]
    for copy in copies:
        copy.start()
    for copy in copies:
        copy.wait()


def solution(mesh):
    n_dp, n_row, n_x = mesh.shape["dp"], mesh.shape["row"], mesh.shape["fsdp"] // 2

    def local_step(x_dev, dy_dev, gate, up_w, down, g_dev):
        micro, tokens, d_model = x_dev.shape
        blk = gate.shape[1]
        ff = blk * n_row * n_x * 2
        wide = 3 * 256 + 128
        vmem = pl.BlockSpec(memory_space=pltpu.VMEM)
        hbm = pl.BlockSpec(memory_space=pltpu.HBM)

        def body(*refs):
            kernel(n_dp, n_row, n_x, micro, tokens, d_model, ff, blk, *refs)

        shapes = [((micro, d_model, tokens), BF16), ((3, blk, d_model), F32), ((3, d_model, ff), F32)]
        args = [x_dev.transpose(0, 2, 1), dy_dev.transpose(0, 2, 1), gate.T, up_w.T, down, g_dev[0]]
        args = [pltpu.with_memory_space_constraint(arg, pltpu.HBM) for arg in args]
        parts = pl.pallas_call(
            body,
            in_specs=[hbm] * 6,
            out_specs=[vmem] * 3,
            out_shape=[pltpu.VMEM(*shape) for shape in shapes],
            scratch_shapes=[
                pltpu.VMEM((micro, d_model, tokens), BF16),
                pltpu.VMEM((micro, d_model, tokens), BF16),
                pltpu.VMEM((3, d_model, ff), F32),
                pltpu.VMEM((3, blk, d_model), BF16),
                pltpu.VMEM((n_row, n_x, 2, blk, wide), BF16),
                pltpu.VMEM((12 * blk, d_model), BF16),
                pltpu.VMEM((12 * blk, d_model), BF16),
                pltpu.VMEM((12 * blk, d_model), BF16),
                pltpu.VMEM((d_model, ff), BF16),
                pltpu.VMEM((d_model, ff), BF16),
                pltpu.VMEM((ff, micro * tokens), BF16),
                pltpu.VMEM((ff, micro * tokens), BF16),
                pltpu.VMEM((ff, micro * tokens), BF16),
                pltpu.VMEM((n_row, n_x, 2, blk, wide), BF16),
                pltpu.VMEM((n_row, n_x, blk, wide), BF16),
                pltpu.VMEM((n_row, n_x, blk, wide), BF16),
                pltpu.VMEM((2, 2, blk, wide), BF16),
                pltpu.VMEM((2, 2, blk, wide), BF16),
                pltpu.VMEM((2, 2, blk, wide), BF16),
                pltpu.VMEM((2, 2, blk, wide), BF16),
                pltpu.VMEM((4, blk, wide), BF16),
                pltpu.VMEM((3, blk, wide), BF16),
                pltpu.VMEM((blk, wide), BF16),
                pltpu.VMEM((n_dp, blk, wide), BF16),
                pltpu.SemaphoreType.DMA((5,)),
                pltpu.SemaphoreType.DMA((3,)),
                pltpu.SemaphoreType.DMA((31,)),
                pltpu.SemaphoreType.DMA((31,)),
                pltpu.SemaphoreType.DMA((13,)),
                pltpu.SemaphoreType.DMA((13,)),
            ],
            compiler_params=pltpu.CompilerParams(
                collective_id=0, has_side_effects=True, vmem_limit_bytes=54 * 2**20),
            name="mlp_step",
        )(*args)
        dx_t, gn, dw = pl.pallas_call(
            write_out,
            in_specs=[vmem] * 3,
            out_specs=[hbm] * 3,
            out_shape=[jax.ShapeDtypeStruct(*shape) for shape in shapes],
            scratch_shapes=[pltpu.SemaphoreType.DMA((3,))],
            compiler_params=pltpu.CompilerParams(vmem_limit_bytes=2 * 2**20),
            name="write_out",
        )(*parts)
        return dx_t.transpose(0, 2, 1), gn.transpose(0, 2, 1), dw[None]

    in_specs = (P(None, TOK_AXES, None), P(None, TOK_AXES, None), P(None, GROUP_AXES), P(None, GROUP_AXES), P(GROUP_AXES, None), P(TOK_AXES, None, None, None))
    out_specs = (P(None, TOK_AXES, None), P(None, None, GROUP_AXES), P(TOK_AXES, None, None, None))
    return jax.shard_map(local_step, mesh=mesh, in_specs=in_specs, out_specs=out_specs, check_vma=False)
```

```python
import jax
import jax.numpy as jnp
from jax import lax
from jax.experimental import pallas as pl
from jax.experimental.pallas import tpu as pltpu
from jax.sharding import PartitionSpec as P

TOK_AXES = ("dp", "row", "fsdp")
GROUP_AXES = ("row", "fsdp")
F32, BF16 = jnp.float32, jnp.bfloat16
MESH = pl.DeviceIdType.MESH
NN = (((1,), (0,)), ((), ()))
NT = (((1,), (1,)), ((), ()))


def mm(lhs, rhs, dims=NN):
    return lax.dot_general(lhs, rhs, dims, preferred_element_type=F32)


def kernel(n_dp, n_row, n_x, micro, tokens, d_model, ff, blk,
           x_hbm, dy_hbm, w1_hbm, w3_hbm, w2_hbm, g_hbm,
           dx0, acc, x1, dy1, h1, da1, db1, w1, w3, r,
           x0, dy0, h0, da0, db0, g_v, shard, wbuf, g1, g3, g2,
           gt, pr, part, rx1, rx0, mid, rx2, q, ry,
           load_sem, g_sem, ag_s, ag_r, rs_s, rs_r):
    z, y, f = lax.axis_index("dp"), lax.axis_index("row"), lax.axis_index("fsdp")
    x, c = f // 2, f % 2
    main, tail = 256, d_model - 256
    side = n_x
    rows = 2 * blk

    def chip(du, dv):
        return (y + dv * (1 - c) + du * c + side) % side, (x + du * (1 - c) + dv * c + side) % side

    def device(du, dv):
        yy, xx = chip(du, dv)
        return (z, yy, xx * 2 + c)

    partner = (z, y, x * 2 + 1 - c)
    peers = [partner, device(1, 0), device(-1, 0), device(0, 1), device(0, -1), device(0, 2), device(2, 0)]

    barrier = pltpu.get_barrier_semaphore()
    for peer in peers:
        pl.semaphore_signal(barrier, inc=1, device_id=peer, device_id_type=MESH)

    g_loads = [pltpu.make_async_copy(g_hbm.at[s], g_v.at[s], g_sem.at[s]) for s in range(3)]
    t_loads = [[pltpu.make_async_copy(src.at[m], dst[m], load_sem.at[3 + 2 * m + i])
                for i, (src, dst) in enumerate(((x_hbm, (x0, x1)), (dy_hbm, (dy0, dy1))))] for m in range(micro)]
    w_loads = [pltpu.make_async_copy(w, shard.at[i], load_sem.at[i]) for i, w in enumerate((w1_hbm, w3_hbm, w2_hbm))]
    for load in w_loads + t_loads[0] + g_loads + t_loads[1]:
        load.start()
    for load in w_loads:
        load.wait()

    s1, s3, s2 = shard[0], shard[1], shard[2]
    wbuf[y, x, c, :, :main] = s1[:, :main]
    wbuf[y, x, c, :, main:2 * main] = s3[:, :main]
    wbuf[y, x, c, :, 2 * main:3 * main] = s2[:, :main]
    tails = [s[:, main:].astype(F32) for s in (s1, s3, s2)] + [jnp.zeros((blk, 128 - 3 * tail), F32)]
    wbuf[y, x, c, :, 3 * main:] = jnp.concatenate(tails, axis=1).astype(BF16)

    pl.semaphore_wait(barrier, len(peers))

    sent = []
    count = {"ag": 0, "rs": 0}

    def send(kind, src, dst, where):
        i = count[kind]
        count[kind] += 1
        ss, rr = (ag_s, ag_r) if kind == "ag" else (rs_s, rs_r)
        copy = pltpu.make_async_remote_copy(
            src_ref=src, dst_ref=dst, send_sem=ss.at[i], recv_sem=rr.at[i],
            device_id=where, device_id_type=MESH)
        copy.start()
        sent.append(copy)
        return copy

    arrive, pairs = {}, {}

    def forward(du, dv, su, sv):
        ref = wbuf.at[(*chip(du, dv), c)]
        got = tuple((a - b + 1) % side - 1 for a, b in ((du, su), (dv, sv)))
        arrive[got] = send("ag", ref, ref, device(su, sv))

    def share(du, dv):
        ref = wbuf.at[(*chip(du, dv), c)]
        pairs[du, dv] = send("ag", ref, ref, partner)

    def take(du, dv, *steps):
        arrive[du, dv].wait_recv()
        for su, sv in steps:
            forward(du, dv, su, sv)
        share(du, dv)

    for su, sv in ((1, 0), (-1, 0), (0, 1), (0, -1), (2, 0)):
        forward(0, 0, su, sv)
    share(0, 0)

    def turn(s):
        g_loads[s].wait()
        flat = g_v[s, :main, :].T.reshape(n_row, n_x, 2, blk, main)
        gt[..., s * main:(s + 1) * main] = flat.astype(BF16)

    def turn_tail():
        parts = [g_v[s, main:, :] for s in range(3)] + [jnp.zeros((128 - 3 * tail, ff), F32)]
        flat = jnp.concatenate(parts, axis=0).T.reshape(n_row, n_x, 2, blk, 128)
        gt[..., 3 * main:] = flat.astype(BF16)

    def fill(group):
        for j, (du, dv) in enumerate(group):
            both = wbuf[chip(du, dv)].astype(F32).reshape(rows, 3 * main + 128).astype(BF16)
            at = slice(j * rows, (j + 1) * rows)
            for i, ref in enumerate((g1, g3, g2)):
                ref[at, :main] = both[:, i * main:(i + 1) * main]
                ref[at, main:] = both[:, 3 * main + i * tail:3 * main + (i + 1) * tail]

    def ahead(group, m, lo=0, hi=tokens):
        n = len(group) * rows
        xt, dyt = ((x0, dy0), (x1, dy1))[m]
        xt, dyt = xt[:, lo:hi], dyt[:, lo:hi]
        a, b, dh = mm(g1[:n], xt), mm(g3[:n], xt), mm(g2[:n], dyt)
        sig = 0.5 * jnp.tanh(0.5 * a) + 0.5
        act = a * sig
        h = (act * b).astype(BF16)
        db = (dh * act).astype(BF16)
        da = (dh * b * (sig + act * (1.0 - sig))).astype(BF16)
        for j, (du, dv) in enumerate(group):
            yy, xx = chip(du, dv)
            to = pl.ds(pl.multiple_of((yy * n_x + xx) * rows, 16), rows)
            at = slice(j * rows, (j + 1) * rows)
            for ref, value in zip(((h0, da0, db0), (h1, da1, db1))[m], (h, da, db)):
                ref[to, lo:hi] = value[at]

    for load in t_loads[0]:
        load.wait()
    pairs[0, 0].wait_recv()
    fill([(0, 0)])
    ahead([(0, 0)], 0)
    turn(0)
    turn(1)
    turn(2)
    turn_tail()

    take(-1, 0, (0, 1), (0, -1))
    take(1, 0, (0, 1), (0, -1))
    take(0, 1, (0, -1))
    take(0, -1)
    for load in t_loads[1]:
        load.wait()
    ahead([(0, 0)], 1)
    near = [(-1, 0), (1, 0), (0, -1), (0, 1)]
    take(2, 0, (0, 1), (0, -1))
    for key in near:
        pairs[key].wait_recv()
    pair = send("rs", gt.at[:, :, 1 - c], pr, partner)
    fill(near)
    ahead(near, 0)
    ahead(near, 1, 0, tokens // 2)
    pair.wait_recv()
    for yy in range(n_row):
        for xx in range(n_x):
            both = gt[yy, xx, c].astype(F32) + pr[yy, xx].astype(F32)
            part[xx * (1 - c) + yy * c, yy * (1 - c) + xx * c] = both.astype(BF16)
    u, v = x * (1 - c) + y * c, y * (1 - c) + x * c
    um, up, uo = (u + side - 1) % side, (u + 1) % side, (u + 2) % side
    lo, hi = pl.ds(0, side // 2), pl.ds(side // 2, side // 2)

    take(-1, -1, (0, 1))
    take(1, 1, (0, -1))
    take(-1, 1)
    take(1, -1)
    take(0, 2)
    u1 = [send("rs", part.at[uo, lo], rx1.at[0], device(1, 0)),
          send("rs", part.at[uo, hi], rx1.at[1], device(-1, 0))]
    ahead(near, 1, tokens // 2)
    mids = [(2, 0), (0, 2), (-1, -1), (1, 1), (-1, 1), (1, -1)]
    for key in mids:
        pairs[key].wait_recv()
    fill(mids)
    ahead(mids, 0)
    take(2, 1, (0, -1))
    take(2, -1)
    take(-1, 2)
    take(1, 2)
    u0 = [send("rs", part.at[up, hi], rx0.at[0], device(1, 0)),
          send("rs", part.at[um, lo], rx0.at[1], device(-1, 0))]
    ahead(mids, 1)

    for copy in u1:
        copy.wait_recv()
    half = side // 2
    mid[0] = (part[up, :half].astype(F32) + rx1[0].astype(F32)).astype(BF16)
    mid[1] = (part[um, half:].astype(F32) + rx1[1].astype(F32)).astype(BF16)
    u2 = [send("rs", mid.at[0], rx2.at[0], device(1, 0)), send("rs", mid.at[1], rx2.at[1], device(-1, 0))]

    far = [(2, 1), (2, -1), (-1, 2), (1, 2)]
    for key in far:
        pairs[key].wait_recv()
    fill(far)
    ahead(far, 0)
    take(2, 2)
    ahead(far, 1)
    pairs[2, 2].wait_recv()
    fill([(2, 2)])

    for copy in u0 + u2:
        copy.wait_recv()
    q[:half] = (part[u, :half].astype(F32) + rx2[0].astype(F32) + rx0[1].astype(F32)).astype(BF16)
    q[half:] = (part[u, half:].astype(F32) + rx2[1].astype(F32) + rx0[0].astype(F32)).astype(BF16)
    vs = [send("rs", q.at[(v + d) % side], ry.at[d - 1], device(0, d)) for d in (2, 1, 3)]

    def across(lo, hi):
        return wbuf[..., lo:hi].astype(F32).reshape(ff, hi - lo).astype(BF16).T

    w1[:main, :] = across(0, main)
    w3[:main, :] = across(main, 2 * main)
    ends = across(3 * main, 3 * main + 128)
    w1[main:, :] = ends[:tail]
    w3[main:, :] = ends[tail:2 * tail]

    ahead([(2, 2)], 0)
    dx0[...] = (mm(w1[...], da0[...]) + mm(w3[...], db0[...])).astype(BF16)
    acc[0] = mm(x0[...], da0[...], NT)
    acc[1] = mm(x0[...], db0[...], NT)
    acc[2] = mm(dy0[...], h0[...], NT)
    ahead([(2, 2)], 1)
    for copy in vs:
        copy.wait_recv()
    own = q[v].astype(F32)
    for d in range(1, side):
        own += ry[d - 1].astype(F32)
    r[...] = own.astype(BF16)
    for copy in sent:
        copy.wait_send()


def second(dx0, acc, x1, dy1, h1, da1, db1, w1, w3, dx_hbm, dw_hbm, dx1, dw, sems):
    outs = [pltpu.make_async_copy(dx0, dx_hbm.at[0], sems.at[0]), pltpu.make_async_copy(dx1, dx_hbm.at[1], sems.at[1])]
    outs += [pltpu.make_async_copy(dw.at[s], dw_hbm.at[s], sems.at[2 + s]) for s in range(3)]
    outs[0].start()
    dw[0] = acc[0] + mm(x1[...], da1[...], NT)
    dw[1] = acc[1] + mm(x1[...], db1[...], NT)
    dx1[...] = (mm(w1[...], da1[...]) + mm(w3[...], db1[...])).astype(BF16)
    for i in (2, 3, 1):
        outs[i].start()
    dw[2] = acc[2] + mm(dy1[...], h1[...], NT)
    outs[4].start()
    for out in outs:
        out.wait()


def last(n_dp, main, tail, *refs):
    parts, gn, stack = refs[:n_dp], refs[n_dp], refs[n_dp + 1]
    z = lax.axis_index("dp")
    for d in range(n_dp):
        stack[(z + n_dp - d) % n_dp] = parts[d][...]
    total = stack[0].astype(F32)
    for d in range(1, n_dp):
        total += stack[d].astype(F32)
    for s in range(3):
        gn[s, :, :main] = total[:, s * main:(s + 1) * main]
        gn[s, :, main:] = total[:, 3 * main + s * tail:3 * main + (s + 1) * tail]


def solution(mesh):
    n_dp, n_row, n_x = mesh.shape["dp"], mesh.shape["row"], mesh.shape["fsdp"] // 2

    def local_step(x_dev, dy_dev, gate, up_w, down, g_dev):
        micro, tokens, d_model = x_dev.shape
        blk = gate.shape[1]
        ff = blk * n_row * n_x * 2
        wide = 3 * 256 + 128
        vmem = pl.BlockSpec(memory_space=pltpu.VMEM)
        hbm = pl.BlockSpec(memory_space=pltpu.HBM)

        def body(*refs):
            kernel(n_dp, n_row, n_x, micro, tokens, d_model, ff, blk, *refs)

        args = [x_dev.transpose(0, 2, 1), dy_dev.transpose(0, 2, 1), gate.T, up_w.T, down, g_dev[0]]
        args = [pltpu.with_memory_space_constraint(arg, pltpu.HBM) for arg in args]
        half, mids = (d_model, tokens), (ff, tokens)
        outs = [pltpu.VMEM(half, BF16), pltpu.VMEM((3, d_model, ff), F32)] + [pltpu.VMEM(half, BF16)] * 2
        outs += [pltpu.VMEM(mids, BF16)] * 3 + [pltpu.VMEM((d_model, ff), BF16)] * 2 + [pltpu.VMEM((blk, wide), BF16)]
        *rest, r = pl.pallas_call(
            body,
            in_specs=[hbm] * 6,
            out_specs=[vmem] * len(outs),
            out_shape=outs,
            scratch_shapes=[
                pltpu.VMEM(half, BF16),
                pltpu.VMEM(half, BF16),
                pltpu.VMEM(mids, BF16),
                pltpu.VMEM(mids, BF16),
                pltpu.VMEM(mids, BF16),
                pltpu.VMEM((3, d_model, ff), F32),
                pltpu.VMEM((3, blk, d_model), BF16),
                pltpu.VMEM((n_row, n_x, 2, blk, wide), BF16),
                pltpu.VMEM((12 * blk, d_model), BF16),
                pltpu.VMEM((12 * blk, d_model), BF16),
                pltpu.VMEM((12 * blk, d_model), BF16),
                pltpu.VMEM((n_row, n_x, 2, blk, wide), BF16),
                pltpu.VMEM((n_row, n_x, blk, wide), BF16),
                pltpu.VMEM((n_row, n_x, blk, wide), BF16),
                pltpu.VMEM((2, 2, blk, wide), BF16),
                pltpu.VMEM((2, 2, blk, wide), BF16),
                pltpu.VMEM((2, 2, blk, wide), BF16),
                pltpu.VMEM((2, 2, blk, wide), BF16),
                pltpu.VMEM((4, blk, wide), BF16),
                pltpu.VMEM((3, blk, wide), BF16),
                pltpu.SemaphoreType.DMA((3 + 2 * micro,)),
                pltpu.SemaphoreType.DMA((3,)),
                pltpu.SemaphoreType.DMA((31,)),
                pltpu.SemaphoreType.DMA((31,)),
                pltpu.SemaphoreType.DMA((10,)),
                pltpu.SemaphoreType.DMA((10,)),
            ],
            compiler_params=pltpu.CompilerParams(
                collective_id=0, has_side_effects=True, vmem_limit_bytes=34 * 2**20),
            name="mlp_step",
        )(*args)
        ring = [r] + [lax.ppermute(r, "dp", [(i, (i + d) % n_dp) for i in range(n_dp)]) for d in range(1, n_dp)]
        dx_t, dw = pl.pallas_call(
            second,
            in_specs=[vmem] * len(rest),
            out_specs=[hbm] * 2,
            out_shape=[jax.ShapeDtypeStruct((micro, d_model, tokens), BF16), jax.ShapeDtypeStruct((3, d_model, ff), F32)],
            scratch_shapes=[pltpu.VMEM(half, BF16), pltpu.VMEM((3, d_model, ff), F32), pltpu.SemaphoreType.DMA((5,))],
            compiler_params=pltpu.CompilerParams(vmem_limit_bytes=16 * 2**20),
            cost_estimate=pl.CostEstimate(flops=7 * 10**9, bytes_accessed=5 * 10**6, transcendentals=0),
            name="second",
        )(*rest)

        def finish(*refs):
            last(n_dp, 256, d_model - 256, *refs)

        gn = pl.pallas_call(
            finish,
            in_specs=[vmem] * n_dp,
            out_specs=vmem,
            out_shape=jax.ShapeDtypeStruct((3, blk, d_model), F32),
            scratch_shapes=[pltpu.VMEM((n_dp, blk, wide), BF16)],
            compiler_params=pltpu.CompilerParams(vmem_limit_bytes=4 * 2**20),
            name="last_sum",
        )(*ring)
        return dx_t.transpose(0, 2, 1), gn.transpose(0, 2, 1), dw[None]

    in_specs = (P(None, TOK_AXES, None), P(None, TOK_AXES, None), P(None, GROUP_AXES), P(None, GROUP_AXES), P(GROUP_AXES, None), P(TOK_AXES, None, None, None))
    out_specs = (P(None, TOK_AXES, None), P(None, None, GROUP_AXES), P(TOK_AXES, None, None, None))
    return jax.shard_map(local_step, mesh=mesh, in_specs=in_specs, out_specs=out_specs, check_vma=False)
```

```python
import jax
import jax.numpy as jnp
from jax import lax
from jax.experimental import pallas as pl
from jax.experimental.pallas import tpu as pltpu
from jax.sharding import PartitionSpec as P

TOK_AXES = ("dp", "row", "fsdp")
GROUP_AXES = ("row", "fsdp")
F32, BF16 = jnp.float32, jnp.bfloat16
MESH = pl.DeviceIdType.MESH
NN = (((1,), (0,)), ((), ()))
NT = (((1,), (1,)), ((), ()))


def mm(lhs, rhs, dims=NN):
    return lax.dot_general(lhs, rhs, dims, preferred_element_type=F32)


def kernel(n_dp, n_row, n_x, micro, tokens, d_model, ff, blk,
           x_hbm, dy_hbm, w1_hbm, w3_hbm, w2_hbm, g_hbm,
           dx0, dx1, acc, gn, dy1, h1,
           x0, x1, dy0, h0, da0, da1, db0, db1, w1, w3, g_v, shard, wbuf, g1, g3, g2,
           gt, pr, part, rx1, rx0, mid, rx2, q, ry, r, rz,
           load_sem, g_sem, ag_s, ag_r, rs_s, rs_r, dp_ready):
    z, y, f = lax.axis_index("dp"), lax.axis_index("row"), lax.axis_index("fsdp")
    x, c = f // 2, f % 2
    main, tail = 256, d_model - 256
    side = n_x
    rows = 2 * blk

    def chip(du, dv):
        return (y + dv * (1 - c) + du * c + side) % side, (x + du * (1 - c) + dv * c + side) % side

    def device(du, dv):
        yy, xx = chip(du, dv)
        return (z, yy, xx * 2 + c)

    partner = (z, y, x * 2 + 1 - c)
    peers = [partner, device(1, 0), device(-1, 0), device(0, 1), device(0, -1), device(0, 2), device(2, 0)]

    barrier = pltpu.get_barrier_semaphore()
    for peer in peers:
        pl.semaphore_signal(barrier, inc=1, device_id=peer, device_id_type=MESH)

    for d in range(1, n_dp):
        @pl.when(z + d < n_dp)
        def _():
            pl.semaphore_signal(barrier, inc=1, device_id=(z + d, y, f), device_id_type=MESH)

    g_loads = [pltpu.make_async_copy(g_hbm.at[s], g_v.at[s], g_sem.at[s]) for s in range(3)]
    t_loads = [[pltpu.make_async_copy(src.at[m], dst[m], load_sem.at[3 + 2 * m + i])
                for i, (src, dst) in enumerate(((x_hbm, (x0, x1)), (dy_hbm, (dy0, dy1))))] for m in range(micro)]
    w_loads = [pltpu.make_async_copy(w, shard.at[i], load_sem.at[i]) for i, w in enumerate((w1_hbm, w3_hbm, w2_hbm))]
    for load in w_loads + t_loads[0] + g_loads + t_loads[1]:
        load.start()
    for load in w_loads:
        load.wait()

    s1, s3, s2 = shard[0], shard[1], shard[2]
    wbuf[y, x, c, :, :main] = s1[:, :main]
    wbuf[y, x, c, :, main:2 * main] = s3[:, :main]
    wbuf[y, x, c, :, 2 * main:3 * main] = s2[:, :main]
    tails = [s[:, main:].astype(F32) for s in (s1, s3, s2)] + [jnp.zeros((blk, 128 - 3 * tail), F32)]
    wbuf[y, x, c, :, 3 * main:] = jnp.concatenate(tails, axis=1).astype(BF16)

    pl.semaphore_wait(barrier, len(peers) + z)
    for d in range(1, n_dp):
        @pl.when(z >= d)
        def _():
            pl.semaphore_signal(dp_ready, inc=1, device_id=(z - d, y, f), device_id_type=MESH)

    sent = []
    count = {"ag": 0, "rs": 0}

    def send(kind, src, dst, where):
        i = count[kind]
        count[kind] += 1
        ss, rr = (ag_s, ag_r) if kind == "ag" else (rs_s, rs_r)
        copy = pltpu.make_async_remote_copy(
            src_ref=src, dst_ref=dst, send_sem=ss.at[i], recv_sem=rr.at[i],
            device_id=where, device_id_type=MESH)
        copy.start()
        sent.append(copy)
        return copy

    arrive, pairs = {}, {}

    def forward(du, dv, su, sv):
        ref = wbuf.at[(*chip(du, dv), c)]
        got = tuple((a - b + 1) % side - 1 for a, b in ((du, su), (dv, sv)))
        arrive[got] = send("ag", ref, ref, device(su, sv))

    def share(du, dv):
        ref = wbuf.at[(*chip(du, dv), c)]
        pairs[du, dv] = send("ag", ref, ref, partner)

    def take(du, dv, *steps):
        arrive[du, dv].wait_recv()
        for su, sv in steps:
            forward(du, dv, su, sv)
        share(du, dv)

    for su, sv in ((1, 0), (-1, 0), (0, 1), (0, -1), (2, 0)):
        forward(0, 0, su, sv)
    share(0, 0)

    def turn(s):
        g_loads[s].wait()
        flat = g_v[s, :main, :].T.reshape(n_row, n_x, 2, blk, main)
        gt[..., s * main:(s + 1) * main] = flat.astype(BF16)

    def turn_tail():
        parts = [g_v[s, main:, :] for s in range(3)] + [jnp.zeros((128 - 3 * tail, ff), F32)]
        flat = jnp.concatenate(parts, axis=0).T.reshape(n_row, n_x, 2, blk, 128)
        gt[..., 3 * main:] = flat.astype(BF16)

    def fill(group):
        for j, (du, dv) in enumerate(group):
            both = wbuf[chip(du, dv)].astype(F32).reshape(rows, 3 * main + 128).astype(BF16)
            at = slice(j * rows, (j + 1) * rows)
            for i, ref in enumerate((g1, g3, g2)):
                ref[at, :main] = both[:, i * main:(i + 1) * main]
                ref[at, main:] = both[:, 3 * main + i * tail:3 * main + (i + 1) * tail]

    def ahead(group, m, lo=0, hi=tokens):
        n = len(group) * rows
        xt, dyt = ((x0, dy0), (x1, dy1))[m]
        xt, dyt = xt[:, lo:hi], dyt[:, lo:hi]
        a, b, dh = mm(g1[:n], xt), mm(g3[:n], xt), mm(g2[:n], dyt)
        sig = 0.5 * jnp.tanh(0.5 * a) + 0.5
        act = a * sig
        h = (act * b).astype(BF16)
        db = (dh * act).astype(BF16)
        da = (dh * b * (sig + act * (1.0 - sig))).astype(BF16)
        for j, (du, dv) in enumerate(group):
            yy, xx = chip(du, dv)
            to = pl.ds(pl.multiple_of((yy * n_x + xx) * rows, 16), rows)
            at = slice(j * rows, (j + 1) * rows)
            for ref, value in zip(((h0, da0, db0), (h1, da1, db1))[m], (h, da, db)):
                ref[to, lo:hi] = value[at]

    for load in t_loads[0]:
        load.wait()
    pairs[0, 0].wait_recv()
    fill([(0, 0)])
    ahead([(0, 0)], 0)
    turn(0)
    turn(1)
    turn(2)
    turn_tail()

    take(-1, 0, (0, 1), (0, -1))
    take(1, 0, (0, 1), (0, -1))
    take(0, 1, (0, -1))
    take(0, -1)
    for load in t_loads[1]:
        load.wait()
    ahead([(0, 0)], 1)
    near = [(-1, 0), (1, 0), (0, -1), (0, 1)]
    take(2, 0, (0, 1), (0, -1))
    for key in near:
        pairs[key].wait_recv()
    pair = send("rs", gt.at[:, :, 1 - c], pr, partner)
    fill(near)
    ahead(near, 0)
    ahead(near, 1, 0, tokens // 2)
    pair.wait_recv()
    for yy in range(n_row):
        for xx in range(n_x):
            both = gt[yy, xx, c].astype(F32) + pr[yy, xx].astype(F32)
            part[xx * (1 - c) + yy * c, yy * (1 - c) + xx * c] = both.astype(BF16)
    u, v = x * (1 - c) + y * c, y * (1 - c) + x * c
    um, up, uo = (u + side - 1) % side, (u + 1) % side, (u + 2) % side
    lo, hi = pl.ds(0, side // 2), pl.ds(side // 2, side // 2)

    take(-1, -1, (0, 1))
    take(1, 1, (0, -1))
    take(-1, 1)
    take(1, -1)
    take(0, 2)
    u1 = [send("rs", part.at[uo, lo], rx1.at[0], device(1, 0)),
          send("rs", part.at[uo, hi], rx1.at[1], device(-1, 0))]
    ahead(near, 1, tokens // 2)
    mids = [(2, 0), (0, 2), (-1, -1), (1, 1), (-1, 1), (1, -1)]
    for key in mids:
        pairs[key].wait_recv()
    fill(mids)
    ahead(mids, 0)
    take(2, 1, (0, -1))
    take(2, -1)
    take(-1, 2)
    take(1, 2)
    for copy in u1:
        copy.wait_recv()
    half = side // 2
    mid[0] = (part[up, :half].astype(F32) + rx1[0].astype(F32)).astype(BF16)
    mid[1] = (part[um, half:].astype(F32) + rx1[1].astype(F32)).astype(BF16)
    u2 = [send("rs", mid.at[0], rx2.at[0], device(1, 0)), send("rs", mid.at[1], rx2.at[1], device(-1, 0))]
    u0 = [send("rs", part.at[up, hi], rx0.at[0], device(1, 0)),
          send("rs", part.at[um, lo], rx0.at[1], device(-1, 0))]
    ahead(mids, 1)

    far = [(2, 1), (2, -1), (-1, 2), (1, 2)]
    for key in far:
        pairs[key].wait_recv()
    fill(far)
    ahead(far, 0)
    take(2, 2)
    for copy in u0 + u2:
        copy.wait_recv()
    q[:half] = (part[u, :half].astype(F32) + rx2[0].astype(F32) + rx0[1].astype(F32)).astype(BF16)
    q[half:] = (part[u, half:].astype(F32) + rx2[1].astype(F32) + rx0[0].astype(F32)).astype(BF16)
    vs = [send("rs", q.at[(v + d) % side], ry.at[d - 1], device(0, d)) for d in (2, 1, 3)]
    ahead(far, 1)
    pairs[2, 2].wait_recv()
    fill([(2, 2)])

    def across(lo, hi):
        return wbuf[..., lo:hi].astype(F32).reshape(ff, hi - lo).astype(BF16).T

    w1[:main, :] = across(0, main)
    w3[:main, :] = across(main, 2 * main)
    ends = across(3 * main, 3 * main + 128)
    w1[main:, :] = ends[:tail]
    w3[main:, :] = ends[tail:2 * tail]

    cut = tokens // 2
    for m, (x_m, dy_m, h_m, da_m, db_m, dx_m) in enumerate(((x0, dy0, h0, da0, db0, dx0), (x1, dy1, h1, da1, db1, dx1))):
        ahead([(2, 2)], m)
        for lo, hi in ((0, cut), (cut, tokens)) if m == 0 else ((0, tokens),):
            da, db = da_m[:, lo:hi], db_m[:, lo:hi]
            dx_m[:, lo:hi] = (mm(w1[...], da) + mm(w3[...], db)).astype(BF16)
            first = m == 0 and lo == 0
            acc[0] = (0 if first else acc[0]) + mm(x_m[:, lo:hi], da, NT)
            acc[1] = (0 if first else acc[1]) + mm(x_m[:, lo:hi], db, NT)
            if m == 0:
                acc[2] = (0 if first else acc[2]) + mm(dy_m[:, lo:hi], h_m[:, lo:hi], NT)
            if first:
                for copy in vs:
                    copy.wait_recv()
                own = q[v].astype(F32)
                for d in range(1, side):
                    own += ry[d - 1].astype(F32)
                r[...] = own.astype(BF16)

                @pl.when(z < n_dp - 1)
                def _():
                    pl.semaphore_wait(dp_ready, n_dp - 1 - z)

                zs = [send("rs", r, rz.at[z], ((z + d) % n_dp, y, f)) for d in (2, 1, 3)]
                rz[z] = r[...]
    for copy in zs:
        copy.wait_recv()
    total = rz[0].astype(F32)
    for d in range(1, n_dp):
        total += rz[d].astype(F32)
    for s in range(3):
        gn[s, :, :main] = total[:, s * main:(s + 1) * main]
        gn[s, :, main:] = total[:, 3 * main + s * tail:3 * main + (s + 1) * tail]
    for copy in sent:
        copy.wait_send()


def second(dx0, dx1, acc, gn, dy1, h1, dx_hbm, gn_hbm, dw_hbm, dw, sems):
    moves = [(dx0, dx_hbm.at[0]), (dx1, dx_hbm.at[1]), (acc.at[0], dw_hbm.at[0]), (acc.at[1], dw_hbm.at[1]), (gn, gn_hbm), (dw, dw_hbm.at[2])]
    outs = [pltpu.make_async_copy(src, dst, sems.at[i]) for i, (src, dst) in enumerate(moves)]
    for out in outs[:-1]:
        out.start()
    dw[...] = acc[2] + mm(dy1[...], h1[...], NT)
    outs[-1].start()
    for out in outs:
        out.wait()


def solution(mesh):
    n_dp, n_row, n_x = mesh.shape["dp"], mesh.shape["row"], mesh.shape["fsdp"] // 2

    def local_step(x_dev, dy_dev, gate, up_w, down, g_dev):
        micro, tokens, d_model = x_dev.shape
        blk = gate.shape[1]
        ff = blk * n_row * n_x * 2
        wide = 3 * 256 + 128
        vmem = pl.BlockSpec(memory_space=pltpu.VMEM)
        hbm = pl.BlockSpec(memory_space=pltpu.HBM)

        def body(*refs):
            kernel(n_dp, n_row, n_x, micro, tokens, d_model, ff, blk, *refs)

        args = [x_dev.transpose(0, 2, 1), dy_dev.transpose(0, 2, 1), gate.T, up_w.T, down, g_dev[0]]
        args = [pltpu.with_memory_space_constraint(arg, pltpu.HBM) for arg in args]
        half, mids = (d_model, tokens), (ff, tokens)
        outs = [pltpu.VMEM(half, BF16)] * 2 + [pltpu.VMEM((3, d_model, ff), F32), pltpu.VMEM((3, blk, d_model), F32)]
        outs += [pltpu.VMEM(half, BF16), pltpu.VMEM(mids, BF16)]
        parts = pl.pallas_call(
            body,
            in_specs=[hbm] * 6,
            out_specs=[vmem] * len(outs),
            out_shape=outs,
            scratch_shapes=[
                *[pltpu.VMEM(half, BF16)] * 3,
                *[pltpu.VMEM(mids, BF16)] * 5,
                *[pltpu.VMEM((d_model, ff), BF16)] * 2,
                pltpu.VMEM((3, d_model, ff), F32),
                pltpu.VMEM((3, blk, d_model), BF16),
                pltpu.VMEM((n_row, n_x, 2, blk, wide), BF16),
                pltpu.VMEM((12 * blk, d_model), BF16),
                pltpu.VMEM((12 * blk, d_model), BF16),
                pltpu.VMEM((12 * blk, d_model), BF16),
                pltpu.VMEM((n_row, n_x, 2, blk, wide), BF16),
                pltpu.VMEM((n_row, n_x, blk, wide), BF16),
                pltpu.VMEM((n_row, n_x, blk, wide), BF16),
                pltpu.VMEM((2, 2, blk, wide), BF16),
                pltpu.VMEM((2, 2, blk, wide), BF16),
                pltpu.VMEM((2, 2, blk, wide), BF16),
                pltpu.VMEM((2, 2, blk, wide), BF16),
                pltpu.VMEM((4, blk, wide), BF16),
                pltpu.VMEM((3, blk, wide), BF16),
                pltpu.VMEM((blk, wide), BF16),
                pltpu.VMEM((n_dp, blk, wide), BF16),
                pltpu.SemaphoreType.DMA((3 + 2 * micro,)),
                pltpu.SemaphoreType.DMA((3,)),
                pltpu.SemaphoreType.DMA((31,)),
                pltpu.SemaphoreType.DMA((31,)),
                pltpu.SemaphoreType.DMA((13,)),
                pltpu.SemaphoreType.DMA((13,)),
                pltpu.SemaphoreType.REGULAR,
            ],
            compiler_params=pltpu.CompilerParams(
                collective_id=0, has_side_effects=True, vmem_limit_bytes=44 * 2**20),
            name="mlp_step",
        )(*args)
        dx_t, gn, dw = pl.pallas_call(
            second,
            in_specs=[vmem] * len(parts),
            out_specs=[hbm] * 3,
            out_shape=[jax.ShapeDtypeStruct(shape, dtype) for shape, dtype in
                       (((micro, d_model, tokens), BF16), ((3, blk, d_model), F32), ((3, d_model, ff), F32))],
            scratch_shapes=[pltpu.VMEM((d_model, ff), F32), pltpu.SemaphoreType.DMA((6,))],
            compiler_params=pltpu.CompilerParams(vmem_limit_bytes=12 * 2**20),
            name="second",
        )(*parts)
        return dx_t.transpose(0, 2, 1), gn.transpose(0, 2, 1), dw[None]

    in_specs = (P(None, TOK_AXES, None), P(None, TOK_AXES, None), P(None, GROUP_AXES), P(None, GROUP_AXES), P(GROUP_AXES, None), P(TOK_AXES, None, None, None))
    out_specs = (P(None, TOK_AXES, None), P(None, None, GROUP_AXES), P(TOK_AXES, None, None, None))
    return jax.shard_map(local_step, mesh=mesh, in_specs=in_specs, out_specs=out_specs, check_vma=False)
```

```python
import jax
import jax.numpy as jnp
from jax import lax
from jax.experimental import pallas as pl
from jax.experimental.pallas import tpu as pltpu
from jax.sharding import PartitionSpec as P

TOK_AXES = ("dp", "row", "fsdp")
GROUP_AXES = ("row", "fsdp")
F32, BF16 = jnp.float32, jnp.bfloat16
MESH = pl.DeviceIdType.MESH
NN = (((1,), (0,)), ((), ()))
NT = (((1,), (1,)), ((), ()))


def mm(lhs, rhs, dims=NN):
    return lax.dot_general(lhs, rhs, dims, preferred_element_type=F32)


def kernel(n_dp, n_row, n_x, micro, tokens, d_model, ff, blk,
           x_hbm, dy_hbm, w1_hbm, w3_hbm, w2_hbm, g_hbm,
           dx0, dx1, acc, gn, x1, dy1, h1, da1, db1,
           x0, dy0, h0, da0, db0, w1, w3, g_v, shard, wbuf, g1, g3, g2,
           gt, pr, part, rx1, rx0, mid, rx2, q, ry, r, rz,
           load_sem, g_sem, ag_s, ag_r, rs_s, rs_r, dp_ready, ready):
    z, y, f = lax.axis_index("dp"), lax.axis_index("row"), lax.axis_index("fsdp")
    x, c = f // 2, f % 2
    main, tail = 256, d_model - 256
    side = n_x
    rows = 2 * blk

    def chip(du, dv):
        return (y + dv * (1 - c) + du * c + side) % side, (x + du * (1 - c) + dv * c + side) % side

    def device(du, dv):
        yy, xx = chip(du, dv)
        return (z, yy, xx * 2 + c)

    partner = (z, y, x * 2 + 1 - c)
    rank = y * 2 * n_x + f
    near_by = [(1, 0), (-1, 0), (0, 1), (0, -1), (2, 0), (0, 2)]
    peers = [(device(du, dv), k) for k, (du, dv) in enumerate(near_by)] + [(partner, 6)]
    back_to = [1, 0, 3, 2, 4, 5, 6]

    def rank_of(peer):
        return peer[1] * 2 * n_x + peer[2]

    barrier = pltpu.get_barrier_semaphore()
    lower = z
    for peer, k in peers:
        lower += (rank_of(peer) < rank).astype(jnp.int32)

        @pl.when(rank_of(peer) > rank)
        def _():
            pl.semaphore_signal(barrier, inc=1, device_id=peer, device_id_type=MESH)

    for d in range(1, n_dp):
        @pl.when(z + d < n_dp)
        def _():
            pl.semaphore_signal(barrier, inc=1, device_id=(z + d, y, f), device_id_type=MESH)

    g_loads = [pltpu.make_async_copy(g_hbm.at[s], g_v.at[s], g_sem.at[s]) for s in range(3)]
    t_loads = [[pltpu.make_async_copy(src.at[m], dst[m], load_sem.at[3 + 2 * m + i])
                for i, (src, dst) in enumerate(((x_hbm, (x0, x1)), (dy_hbm, (dy0, dy1))))] for m in range(micro)]
    w_loads = [pltpu.make_async_copy(w, shard.at[i], load_sem.at[i]) for i, w in enumerate((w1_hbm, w3_hbm, w2_hbm))]
    for load in w_loads + t_loads[0] + g_loads + t_loads[1]:
        load.start()
    for load in w_loads:
        load.wait()

    s1, s3, s2 = shard[0], shard[1], shard[2]
    wbuf[y, x, c, :, :main] = s1[:, :main]
    wbuf[y, x, c, :, main:2 * main] = s3[:, :main]
    wbuf[y, x, c, :, 2 * main:3 * main] = s2[:, :main]
    tails = [s[:, main:].astype(F32) for s in (s1, s3, s2)] + [jnp.zeros((blk, 128 - 3 * tail), F32)]
    wbuf[y, x, c, :, 3 * main:] = jnp.concatenate(tails, axis=1).astype(BF16)

    @pl.when(lower > 0)
    def _():
        pl.semaphore_wait(barrier, lower)

    for peer, k in peers:
        @pl.when(rank_of(peer) < rank)
        def _():
            pl.semaphore_signal(ready.at[back_to[k]], inc=1, device_id=peer, device_id_type=MESH)

    for d in range(1, n_dp):
        @pl.when(z >= d)
        def _():
            pl.semaphore_signal(dp_ready, inc=1, device_id=(z - d, y, f), device_id_type=MESH)

    sent = []
    count = {"ag": 0, "rs": 0}

    def send(kind, src, dst, where, start=True):
        i = count[kind]
        count[kind] += 1
        ss, rr = (ag_s, ag_r) if kind == "ag" else (rs_s, rs_r)
        copy = pltpu.make_async_remote_copy(
            src_ref=src, dst_ref=dst, send_sem=ss.at[i], recv_sem=rr.at[i],
            device_id=where, device_id_type=MESH)
        if start:
            copy.start()
        sent.append(copy)
        return copy

    arrive, pairs = {}, {}

    def forward(du, dv, su, sv):
        ref = wbuf.at[(*chip(du, dv), c)]
        got = tuple((a - b + 1) % side - 1 for a, b in ((du, su), (dv, sv)))
        arrive[got] = send("ag", ref, ref, device(su, sv))

    def share(du, dv):
        ref = wbuf.at[(*chip(du, dv), c)]
        pairs[du, dv] = send("ag", ref, ref, partner)

    def take(du, dv, *steps):
        arrive[du, dv].wait_recv()
        for su, sv in steps:
            forward(du, dv, su, sv)
        share(du, dv)

    own_block = wbuf.at[y, x, c]
    firsts = {}
    for k in (0, 1, 2, 3, 6, 4):
        firsts[k] = send("ag", own_block, own_block, peers[k][0], start=False)
    arrive.update({(-1, 0): firsts[0], (1, 0): firsts[1], (0, -1): firsts[2], (0, 1): firsts[3], (2, 0): firsts[4]})
    pairs[0, 0] = firsts[6]

    for k, copy in firsts.items():
        @pl.when(rank_of(peers[k][0]) < rank)
        def _():
            copy.start()

    for k, copy in firsts.items():
        @pl.when(rank_of(peers[k][0]) > rank)
        def _():
            pl.semaphore_wait(ready.at[k], 1)
            copy.start()

    def turn(s):
        g_loads[s].wait()
        flat = g_v[s, :main, :].T.reshape(n_row, n_x, 2, blk, main)
        gt[..., s * main:(s + 1) * main] = flat.astype(BF16)

    def turn_tail():
        parts = [g_v[s, main:, :] for s in range(3)] + [jnp.zeros((128 - 3 * tail, ff), F32)]
        flat = jnp.concatenate(parts, axis=0).T.reshape(n_row, n_x, 2, blk, 128)
        gt[..., 3 * main:] = flat.astype(BF16)

    def fill(group):
        for j, (du, dv) in enumerate(group):
            both = wbuf[chip(du, dv)].astype(F32).reshape(rows, 3 * main + 128).astype(BF16)
            at = slice(j * rows, (j + 1) * rows)
            for i, ref in enumerate((g1, g3, g2)):
                ref[at, :main] = both[:, i * main:(i + 1) * main]
                ref[at, main:] = both[:, 3 * main + i * tail:3 * main + (i + 1) * tail]

    def ahead(group, m, lo=0, hi=tokens):
        n = len(group) * rows
        xt, dyt = ((x0, dy0), (x1, dy1))[m]
        xt, dyt = xt[:, lo:hi], dyt[:, lo:hi]
        a, b, dh = mm(g1[:n], xt), mm(g3[:n], xt), mm(g2[:n], dyt)
        sig = 0.5 * jnp.tanh(0.5 * a) + 0.5
        act = a * sig
        h = (act * b).astype(BF16)
        db = (dh * act).astype(BF16)
        da = (dh * b * (sig + act * (1.0 - sig))).astype(BF16)
        for j, (du, dv) in enumerate(group):
            yy, xx = chip(du, dv)
            to = pl.ds(pl.multiple_of((yy * n_x + xx) * rows, 16), rows)
            at = slice(j * rows, (j + 1) * rows)
            for ref, value in zip(((h0, da0, db0), (h1, da1, db1))[m], (h, da, db)):
                ref[to, lo:hi] = value[at]

    turn(0)
    turn(1)
    turn(2)
    turn_tail()
    pair = send("rs", gt.at[:, :, 1 - c], pr, partner)
    for load in t_loads[0]:
        load.wait()
    pairs[0, 0].wait_recv()
    fill([(0, 0)])
    ahead([(0, 0)], 0)

    take(-1, 0, (0, 1), (0, -1))
    take(1, 0, (0, 1), (0, -1))
    take(0, 1, (0, -1))
    take(0, -1)
    for load in t_loads[1]:
        load.wait()
    ahead([(0, 0)], 1)
    pair.wait_recv()
    for yy in range(n_row):
        for xx in range(n_x):
            both = gt[yy, xx, c].astype(F32) + pr[yy, xx].astype(F32)
            part[xx * (1 - c) + yy * c, yy * (1 - c) + xx * c] = both.astype(BF16)
    u, v = x * (1 - c) + y * c, y * (1 - c) + x * c
    um, up, uo = (u + side - 1) % side, (u + 1) % side, (u + 2) % side
    lo, hi = pl.ds(0, side // 2), pl.ds(side // 2, side // 2)
    near = [(-1, 0), (1, 0), (0, -1), (0, 1)]
    take(2, 0, (0, 1), (0, -1))
    u1 = [send("rs", part.at[uo, lo], rx1.at[0], device(1, 0)),
          send("rs", part.at[uo, hi], rx1.at[1], device(-1, 0))]
    for key in near:
        pairs[key].wait_recv()
    fill(near)
    ahead(near, 0)
    ahead(near, 1, 0, tokens // 2)
    take(-1, -1, (0, 1))
    take(1, 1, (0, -1))
    take(-1, 1)
    take(1, -1)
    take(0, 2)
    u0 = [send("rs", part.at[up, hi], rx0.at[0], device(1, 0)),
          send("rs", part.at[um, lo], rx0.at[1], device(-1, 0))]
    ahead(near, 1, tokens // 2)
    take(2, 1, (0, -1))
    take(2, -1)
    mids = [(2, 0), (0, 2), (-1, -1), (1, 1), (-1, 1), (1, -1)]
    for copy in u1:
        copy.wait_recv()
    half = side // 2
    mid[0] = (part[up, :half].astype(F32) + rx1[0].astype(F32)).astype(BF16)
    mid[1] = (part[um, half:].astype(F32) + rx1[1].astype(F32)).astype(BF16)
    u2 = [send("rs", mid.at[0], rx2.at[0], device(1, 0)), send("rs", mid.at[1], rx2.at[1], device(-1, 0))]
    for key in mids:
        pairs[key].wait_recv()
    fill(mids)
    ahead(mids, 0, 0, tokens * 3 // 4)
    take(-1, 2)
    take(1, 2)
    take(2, 2)
    ahead(mids, 0, tokens * 3 // 4)
    ahead(mids, 1)

    far = [(2, 1), (2, -1), (-1, 2), (1, 2), (2, 2)]
    for key in far:
        pairs[key].wait_recv()
    for copy in u0 + u2:
        copy.wait_recv()
    q[:half] = (part[u, :half].astype(F32) + rx2[0].astype(F32) + rx0[1].astype(F32)).astype(BF16)
    q[half:] = (part[u, half:].astype(F32) + rx2[1].astype(F32) + rx0[0].astype(F32)).astype(BF16)

    @pl.when(rank_of(peers[5][0]) > rank)
    def _():
        pl.semaphore_wait(ready.at[5], 1)

    vs = [send("rs", q.at[(v + d) % side], ry.at[d - 1], device(0, d)) for d in (2, 1, 3)]
    fill(far)
    ahead(far, 0)

    def across(lo, hi):
        return wbuf[..., lo:hi].astype(F32).reshape(ff, hi - lo).astype(BF16).T

    w1[:main, :] = across(0, main)
    w3[:main, :] = across(main, 2 * main)
    ends = across(3 * main, 3 * main + 128)
    w1[main:, :] = ends[:tail]
    w3[main:, :] = ends[tail:2 * tail]
    ahead(far, 1)

    for copy in vs:
        copy.wait_recv()
    own = q[v].astype(F32)
    for d in range(1, side):
        own += ry[d - 1].astype(F32)
    r[...] = own.astype(BF16)

    @pl.when(z < n_dp - 1)
    def _():
        pl.semaphore_wait(dp_ready, n_dp - 1 - z)

    zs = [send("rs", r, rz.at[z], ((z + d) % n_dp, y, f)) for d in (2, 1, 3)]
    rz[z] = r[...]
    dx0[...] = (mm(w1[...], da0[...]) + mm(w3[...], db0[...])).astype(BF16)
    acc[0] = mm(x0[...], da0[...], NT)
    acc[1] = mm(x0[...], db0[...], NT)
    acc[2] = mm(dy0[...], h0[...], NT)
    dx1[...] = (mm(w1[...], da1[...]) + mm(w3[...], db1[...])).astype(BF16)
    for copy in zs:
        copy.wait_recv()
    total = rz[0].astype(F32)
    for d in range(1, n_dp):
        total += rz[d].astype(F32)
    for s in range(3):
        gn[s, :, :main] = total[:, s * main:(s + 1) * main]
        gn[s, :, main:] = total[:, 3 * main + s * tail:3 * main + (s + 1) * tail]
    for copy in sent:
        copy.wait_send()


def second(dx0, dx1, acc, gn, x1, dy1, h1, da1, db1, dx_hbm, gn_hbm, dw_hbm, dw, sems):
    moves = [(dx0, dx_hbm.at[0]), (dx1, dx_hbm.at[1]), (gn, gn_hbm)] + [(dw.at[s], dw_hbm.at[s]) for s in range(3)]
    outs = [pltpu.make_async_copy(src, dst, sems.at[i]) for i, (src, dst) in enumerate(moves)]
    for out in outs[:3]:
        out.start()
    for s, (lhs, rhs) in enumerate(((x1, da1), (x1, db1), (dy1, h1))):
        dw[s] = acc[s] + mm(lhs[...], rhs[...], NT)
        outs[3 + s].start()
    for out in outs:
        out.wait()


def solution(mesh):
    n_dp, n_row, n_x = mesh.shape["dp"], mesh.shape["row"], mesh.shape["fsdp"] // 2

    def local_step(x_dev, dy_dev, gate, up_w, down, g_dev):
        micro, tokens, d_model = x_dev.shape
        blk = gate.shape[1]
        ff = blk * n_row * n_x * 2
        wide = 3 * 256 + 128
        vmem = pl.BlockSpec(memory_space=pltpu.VMEM)
        hbm = pl.BlockSpec(memory_space=pltpu.HBM)

        def body(*refs):
            kernel(n_dp, n_row, n_x, micro, tokens, d_model, ff, blk, *refs)

        args = [x_dev.transpose(0, 2, 1), dy_dev.transpose(0, 2, 1), gate.T, up_w.T, down, g_dev[0]]
        args = [pltpu.with_memory_space_constraint(arg, pltpu.HBM) for arg in args]
        half, mids = (d_model, tokens), (ff, tokens)
        outs = [pltpu.VMEM(half, BF16)] * 2 + [pltpu.VMEM((3, d_model, ff), F32), pltpu.VMEM((3, blk, d_model), F32)]
        outs += [pltpu.VMEM(half, BF16)] * 2 + [pltpu.VMEM(mids, BF16)] * 3
        parts = pl.pallas_call(
            body,
            in_specs=[hbm] * 6,
            out_specs=[vmem] * len(outs),
            out_shape=outs,
            scratch_shapes=[
                *[pltpu.VMEM(half, BF16)] * 2,
                *[pltpu.VMEM(mids, BF16)] * 3,
                *[pltpu.VMEM((d_model, ff), BF16)] * 2,
                pltpu.VMEM((3, d_model, ff), F32),
                pltpu.VMEM((3, blk, d_model), BF16),
                pltpu.VMEM((n_row, n_x, 2, blk, wide), BF16),
                pltpu.VMEM((12 * blk, d_model), BF16),
                pltpu.VMEM((12 * blk, d_model), BF16),
                pltpu.VMEM((12 * blk, d_model), BF16),
                pltpu.VMEM((n_row, n_x, 2, blk, wide), BF16),
                pltpu.VMEM((n_row, n_x, blk, wide), BF16),
                pltpu.VMEM((n_row, n_x, blk, wide), BF16),
                pltpu.VMEM((2, 2, blk, wide), BF16),
                pltpu.VMEM((2, 2, blk, wide), BF16),
                pltpu.VMEM((2, 2, blk, wide), BF16),
                pltpu.VMEM((2, 2, blk, wide), BF16),
                pltpu.VMEM((4, blk, wide), BF16),
                pltpu.VMEM((3, blk, wide), BF16),
                pltpu.VMEM((blk, wide), BF16),
                pltpu.VMEM((n_dp, blk, wide), BF16),
                pltpu.SemaphoreType.DMA((3 + 2 * micro,)),
                pltpu.SemaphoreType.DMA((3,)),
                pltpu.SemaphoreType.DMA((31,)),
                pltpu.SemaphoreType.DMA((31,)),
                pltpu.SemaphoreType.DMA((13,)),
                pltpu.SemaphoreType.DMA((13,)),
                pltpu.SemaphoreType.REGULAR,
                pltpu.SemaphoreType.REGULAR((7,)),
            ],
            compiler_params=pltpu.CompilerParams(
                collective_id=0, has_side_effects=True, vmem_limit_bytes=38 * 2**20),
            name="mlp_step",
        )(*args)
        dx_t, gn, dw = pl.pallas_call(
            second,
            in_specs=[vmem] * len(parts),
            out_specs=[hbm] * 3,
            out_shape=[jax.ShapeDtypeStruct(shape, dtype) for shape, dtype in
                       (((micro, d_model, tokens), BF16), ((3, blk, d_model), F32), ((3, d_model, ff), F32))],
            scratch_shapes=[pltpu.VMEM((3, d_model, ff), F32), pltpu.SemaphoreType.DMA((6,))],
            compiler_params=pltpu.CompilerParams(vmem_limit_bytes=12 * 2**20),
            name="second",
        )(*parts)
        return dx_t.transpose(0, 2, 1), gn.transpose(0, 2, 1), dw[None]

    in_specs = (P(None, TOK_AXES, None), P(None, TOK_AXES, None), P(None, GROUP_AXES), P(None, GROUP_AXES), P(GROUP_AXES, None), P(TOK_AXES, None, None, None))
    out_specs = (P(None, TOK_AXES, None), P(None, None, GROUP_AXES), P(TOK_AXES, None, None, None))
    return jax.shard_map(local_step, mesh=mesh, in_specs=in_specs, out_specs=out_specs, check_vma=False)
```

```python
import jax
import jax.numpy as jnp
from jax import lax
from jax.experimental import pallas as pl
from jax.experimental.pallas import tpu as pltpu
from jax.sharding import PartitionSpec as P

TOK_AXES = ("dp", "row", "fsdp")
GROUP_AXES = ("row", "fsdp")
F32, BF16 = jnp.float32, jnp.bfloat16
MESH = pl.DeviceIdType.MESH
NN = (((1,), (0,)), ((), ()))
NT = (((1,), (1,)), ((), ()))


def mm(lhs, rhs, dims=NN):
    return lax.dot_general(lhs, rhs, dims, preferred_element_type=F32)


def kernel(n_dp, n_row, n_x, micro, tokens, d_model, ff, blk,
           x_hbm, dy_hbm, w1_hbm, w3_hbm, w2_hbm, g_hbm,
           dx0, dx1, acc, gn, x1, dy1, h1, da1, db1,
           x0, dy0, h0, da0, db0, w1, w3, g_v, shard, wbuf, g1, g3, g2,
           gt, pr, part, rx1, rx0, mid, rx2, q, ry, r, rz,
           load_sem, g_sem, ag_s, ag_r, rs_s, rs_r, dp_ready, ready):
    z, y, f = lax.axis_index("dp"), lax.axis_index("row"), lax.axis_index("fsdp")
    x, c = f // 2, f % 2
    main, tail = 256, d_model - 256
    side = n_x
    rows = 2 * blk

    def chip(du, dv):
        return (y + dv * (1 - c) + du * c + side) % side, (x + du * (1 - c) + dv * c + side) % side

    def device(du, dv):
        yy, xx = chip(du, dv)
        return (z, yy, xx * 2 + c)

    partner = (z, y, x * 2 + 1 - c)
    rank = y * 2 * n_x + f
    near_by = [(1, 0), (-1, 0), (0, 1), (0, -1), (2, 0), (0, 2)]
    peers = [(device(du, dv), k) for k, (du, dv) in enumerate(near_by)] + [(partner, 6)]
    back_to = [1, 0, 3, 2, 4, 5, 6]

    def rank_of(peer):
        return peer[1] * 2 * n_x + peer[2]

    barrier = pltpu.get_barrier_semaphore()
    lower = z
    for peer, k in peers:
        lower += (rank_of(peer) < rank).astype(jnp.int32)

        @pl.when(rank_of(peer) > rank)
        def _():
            pl.semaphore_signal(barrier, inc=1, device_id=peer, device_id_type=MESH)

    for d in range(1, n_dp):
        @pl.when(z + d < n_dp)
        def _():
            pl.semaphore_signal(barrier, inc=1, device_id=(z + d, y, f), device_id_type=MESH)

    g_loads = [pltpu.make_async_copy(g_hbm.at[s], g_v.at[s], g_sem.at[s]) for s in range(3)]
    t_loads = [[pltpu.make_async_copy(src.at[m], dst[m], load_sem.at[3 + 2 * m + i])
                for i, (src, dst) in enumerate(((x_hbm, (x0, x1)), (dy_hbm, (dy0, dy1))))] for m in range(micro)]
    w_loads = [pltpu.make_async_copy(w, shard.at[i], load_sem.at[i]) for i, w in enumerate((w1_hbm, w3_hbm, w2_hbm))]
    for load in w_loads + t_loads[0] + g_loads + t_loads[1]:
        load.start()
    for load in w_loads:
        load.wait()

    s1, s3, s2 = shard[0], shard[1], shard[2]
    wbuf[y, x, c, :, :main] = s1[:, :main]
    wbuf[y, x, c, :, main:2 * main] = s3[:, :main]
    wbuf[y, x, c, :, 2 * main:3 * main] = s2[:, :main]
    tails = [s[:, main:].astype(F32) for s in (s1, s3, s2)] + [jnp.zeros((blk, 128 - 3 * tail), F32)]
    wbuf[y, x, c, :, 3 * main:] = jnp.concatenate(tails, axis=1).astype(BF16)

    @pl.when(lower > 0)
    def _():
        pl.semaphore_wait(barrier, lower)

    for peer, k in peers:
        @pl.when(rank_of(peer) < rank)
        def _():
            pl.semaphore_signal(ready.at[back_to[k]], inc=1, device_id=peer, device_id_type=MESH)

    for d in range(1, n_dp):
        @pl.when(z >= d)
        def _():
            pl.semaphore_signal(dp_ready, inc=1, device_id=(z - d, y, f), device_id_type=MESH)

    sent = []
    count = {"ag": 0, "rs": 0}

    def send(kind, src, dst, where, start=True):
        i = count[kind]
        count[kind] += 1
        ss, rr = (ag_s, ag_r) if kind == "ag" else (rs_s, rs_r)
        copy = pltpu.make_async_remote_copy(
            src_ref=src, dst_ref=dst, send_sem=ss.at[i], recv_sem=rr.at[i],
            device_id=where, device_id_type=MESH)
        if start:
            copy.start()
        sent.append(copy)
        return copy

    arrive, pairs = {}, {}

    def forward(du, dv, su, sv):
        ref = wbuf.at[(*chip(du, dv), c)]
        got = tuple((a - b + 1) % side - 1 for a, b in ((du, su), (dv, sv)))
        arrive[got] = send("ag", ref, ref, device(su, sv))

    def share(du, dv):
        ref = wbuf.at[(*chip(du, dv), c)]
        pairs[du, dv] = send("ag", ref, ref, partner)

    def take(du, dv, *steps):
        arrive[du, dv].wait_recv()
        for su, sv in steps:
            forward(du, dv, su, sv)
        share(du, dv)

    own_block = wbuf.at[y, x, c]
    firsts = {}
    for k in (0, 1, 2, 3, 6, 4, 5):
        firsts[k] = send("ag", own_block, own_block, peers[k][0], start=False)
    arrive.update({(-1, 0): firsts[0], (1, 0): firsts[1], (0, -1): firsts[2], (0, 1): firsts[3], (2, 0): firsts[4], (0, 2): firsts[5]})
    pairs[0, 0] = firsts[6]

    for k, copy in firsts.items():
        @pl.when(rank_of(peers[k][0]) < rank)
        def _():
            copy.start()

    for k, copy in firsts.items():
        @pl.when(rank_of(peers[k][0]) > rank)
        def _():
            pl.semaphore_wait(ready.at[k], 1)
            copy.start()

    def turn(s):
        g_loads[s].wait()
        flat = g_v[s, :main, :].T.reshape(n_row, n_x, 2, blk, main)
        gt[..., s * main:(s + 1) * main] = flat.astype(BF16)

    def turn_tail():
        parts = [g_v[s, main:, :] for s in range(3)] + [jnp.zeros((128 - 3 * tail, ff), F32)]
        flat = jnp.concatenate(parts, axis=0).T.reshape(n_row, n_x, 2, blk, 128)
        gt[..., 3 * main:] = flat.astype(BF16)

    def fill(group):
        for j, (du, dv) in enumerate(group):
            both = wbuf[chip(du, dv)].astype(F32).reshape(rows, 3 * main + 128).astype(BF16)
            at = slice(j * rows, (j + 1) * rows)
            for i, ref in enumerate((g1, g3, g2)):
                ref[at, :main] = both[:, i * main:(i + 1) * main]
                ref[at, main:] = both[:, 3 * main + i * tail:3 * main + (i + 1) * tail]

    def ahead(group, m, lo=0, hi=tokens):
        n = len(group) * rows
        xt, dyt = ((x0, dy0), (x1, dy1))[m]
        xt, dyt = xt[:, lo:hi], dyt[:, lo:hi]
        a, b, dh = mm(g1[:n], xt), mm(g3[:n], xt), mm(g2[:n], dyt)
        sig = 0.5 * jnp.tanh(0.5 * a) + 0.5
        act = a * sig
        h = (act * b).astype(BF16)
        db = (dh * act).astype(BF16)
        da = (dh * b * (sig + act * (1.0 - sig))).astype(BF16)
        for j, (du, dv) in enumerate(group):
            yy, xx = chip(du, dv)
            to = pl.ds(pl.multiple_of((yy * n_x + xx) * rows, 16), rows)
            at = slice(j * rows, (j + 1) * rows)
            for ref, value in zip(((h0, da0, db0), (h1, da1, db1))[m], (h, da, db)):
                ref[to, lo:hi] = value[at]

    turn(0)
    turn(1)
    turn(2)
    turn_tail()
    pair = send("rs", gt.at[:, :, 1 - c], pr, partner)
    for load in t_loads[0]:
        load.wait()
    pairs[0, 0].wait_recv()
    fill([(0, 0)])
    ahead([(0, 0)], 0)

    take(-1, 0, (0, 1), (0, -1))
    take(1, 0, (0, 1), (0, -1))
    take(0, 1)
    take(0, -1)
    take(2, 0, (0, 1), (0, -1))
    take(0, 2)
    for load in t_loads[1]:
        load.wait()
    ahead([(0, 0)], 1)
    pair.wait_recv()
    for yy in range(n_row):
        for xx in range(n_x):
            both = gt[yy, xx, c].astype(F32) + pr[yy, xx].astype(F32)
            part[xx * (1 - c) + yy * c, yy * (1 - c) + xx * c] = both.astype(BF16)
    u, v = x * (1 - c) + y * c, y * (1 - c) + x * c
    um, up, uo = (u + side - 1) % side, (u + 1) % side, (u + 2) % side
    lo, hi = pl.ds(0, side // 2), pl.ds(side // 2, side // 2)
    near = [(-1, 0), (1, 0), (0, -1), (0, 1), (2, 0), (0, 2)]
    u1 = [send("rs", part.at[uo, lo], rx1.at[0], device(1, 0)),
          send("rs", part.at[uo, hi], rx1.at[1], device(-1, 0))]
    for key in near:
        pairs[key].wait_recv()
    fill(near)
    ahead(near, 0)
    take(-1, -1, (0, 1))
    take(1, 1, (0, -1))
    take(-1, 1)
    take(1, -1)
    u0 = [send("rs", part.at[up, hi], rx0.at[0], device(1, 0)),
          send("rs", part.at[um, lo], rx0.at[1], device(-1, 0))]
    ahead(near, 1)
    take(2, 1, (0, -1))
    take(2, -1)
    mids = [(-1, -1), (1, 1), (-1, 1), (1, -1)]
    for copy in u1:
        copy.wait_recv()
    half = side // 2
    mid[0] = (part[up, :half].astype(F32) + rx1[0].astype(F32)).astype(BF16)
    mid[1] = (part[um, half:].astype(F32) + rx1[1].astype(F32)).astype(BF16)
    u2 = [send("rs", mid.at[0], rx2.at[0], device(1, 0)), send("rs", mid.at[1], rx2.at[1], device(-1, 0))]
    for key in mids:
        pairs[key].wait_recv()
    fill(mids)
    ahead(mids, 0)
    take(-1, 2)
    take(1, 2)
    take(2, 2)
    ahead(mids, 1)

    far = [(2, 1), (2, -1), (-1, 2), (1, 2), (2, 2)]
    for key in far:
        pairs[key].wait_recv()
    for copy in u0 + u2:
        copy.wait_recv()
    q[:half] = (part[u, :half].astype(F32) + rx2[0].astype(F32) + rx0[1].astype(F32)).astype(BF16)
    q[half:] = (part[u, half:].astype(F32) + rx2[1].astype(F32) + rx0[0].astype(F32)).astype(BF16)

    vs = [send("rs", q.at[(v + d) % side], ry.at[d - 1], device(0, d)) for d in (2, 1, 3)]
    fill(far)
    ahead(far, 0)

    def across(lo, hi):
        return wbuf[..., lo:hi].astype(F32).reshape(ff, hi - lo).astype(BF16).T

    w1[:main, :] = across(0, main)
    w3[:main, :] = across(main, 2 * main)
    ends = across(3 * main, 3 * main + 128)
    w1[main:, :] = ends[:tail]
    w3[main:, :] = ends[tail:2 * tail]
    ahead(far, 1)

    for copy in vs:
        copy.wait_recv()
    own = q[v].astype(F32)
    for d in range(1, side):
        own += ry[d - 1].astype(F32)
    r[...] = own.astype(BF16)

    @pl.when(z < n_dp - 1)
    def _():
        pl.semaphore_wait(dp_ready, n_dp - 1 - z)

    zs = [send("rs", r, rz.at[z], ((z + d) % n_dp, y, f)) for d in (2, 1, 3)]
    rz[z] = r[...]
    dx0[...] = (mm(w1[...], da0[...]) + mm(w3[...], db0[...])).astype(BF16)
    acc[0] = mm(x0[...], da0[...], NT)
    acc[1] = mm(x0[...], db0[...], NT)
    acc[2] = mm(dy0[...], h0[...], NT)
    dx1[...] = (mm(w1[...], da1[...]) + mm(w3[...], db1[...])).astype(BF16)
    for copy in zs:
        copy.wait_recv()
    total = rz[0].astype(F32)
    for d in range(1, n_dp):
        total += rz[d].astype(F32)
    for s in range(3):
        gn[s, :, :main] = total[:, s * main:(s + 1) * main]
        gn[s, :, main:] = total[:, 3 * main + s * tail:3 * main + (s + 1) * tail]
    for copy in sent:
        copy.wait_send()


def second(dx0, dx1, acc, gn, x1, dy1, h1, da1, db1, dx_hbm, gn_hbm, dw_hbm, dw, sems):
    moves = [(dx0, dx_hbm.at[0]), (dx1, dx_hbm.at[1]), (gn, gn_hbm)] + [(dw.at[s], dw_hbm.at[s]) for s in range(3)]
    outs = [pltpu.make_async_copy(src, dst, sems.at[i]) for i, (src, dst) in enumerate(moves)]
    for out in outs[:3]:
        out.start()
    for s, (lhs, rhs) in enumerate(((x1, da1), (x1, db1), (dy1, h1))):
        dw[s] = acc[s] + mm(lhs[...], rhs[...], NT)
        outs[3 + s].start()
    for out in outs:
        out.wait()


def solution(mesh):
    n_dp, n_row, n_x = mesh.shape["dp"], mesh.shape["row"], mesh.shape["fsdp"] // 2

    def local_step(x_dev, dy_dev, gate, up_w, down, g_dev):
        micro, tokens, d_model = x_dev.shape
        blk = gate.shape[1]
        ff = blk * n_row * n_x * 2
        wide = 3 * 256 + 128
        vmem = pl.BlockSpec(memory_space=pltpu.VMEM)
        hbm = pl.BlockSpec(memory_space=pltpu.HBM)

        def body(*refs):
            kernel(n_dp, n_row, n_x, micro, tokens, d_model, ff, blk, *refs)

        args = [x_dev.transpose(0, 2, 1), dy_dev.transpose(0, 2, 1), gate.T, up_w.T, down, g_dev[0]]
        args = [pltpu.with_memory_space_constraint(arg, pltpu.HBM) for arg in args]
        half, mids = (d_model, tokens), (ff, tokens)
        outs = [pltpu.VMEM(half, BF16)] * 2 + [pltpu.VMEM((3, d_model, ff), F32), pltpu.VMEM((3, blk, d_model), F32)]
        outs += [pltpu.VMEM(half, BF16)] * 2 + [pltpu.VMEM(mids, BF16)] * 3
        parts = pl.pallas_call(
            body,
            in_specs=[hbm] * 6,
            out_specs=[vmem] * len(outs),
            out_shape=outs,
            scratch_shapes=[
                *[pltpu.VMEM(half, BF16)] * 2,
                *[pltpu.VMEM(mids, BF16)] * 3,
                *[pltpu.VMEM((d_model, ff), BF16)] * 2,
                pltpu.VMEM((3, d_model, ff), F32),
                pltpu.VMEM((3, blk, d_model), BF16),
                pltpu.VMEM((n_row, n_x, 2, blk, wide), BF16),
                pltpu.VMEM((12 * blk, d_model), BF16),
                pltpu.VMEM((12 * blk, d_model), BF16),
                pltpu.VMEM((12 * blk, d_model), BF16),
                pltpu.VMEM((n_row, n_x, 2, blk, wide), BF16),
                pltpu.VMEM((n_row, n_x, blk, wide), BF16),
                pltpu.VMEM((n_row, n_x, blk, wide), BF16),
                pltpu.VMEM((2, 2, blk, wide), BF16),
                pltpu.VMEM((2, 2, blk, wide), BF16),
                pltpu.VMEM((2, 2, blk, wide), BF16),
                pltpu.VMEM((2, 2, blk, wide), BF16),
                pltpu.VMEM((4, blk, wide), BF16),
                pltpu.VMEM((3, blk, wide), BF16),
                pltpu.VMEM((blk, wide), BF16),
                pltpu.VMEM((n_dp, blk, wide), BF16),
                pltpu.SemaphoreType.DMA((3 + 2 * micro,)),
                pltpu.SemaphoreType.DMA((3,)),
                pltpu.SemaphoreType.DMA((31,)),
                pltpu.SemaphoreType.DMA((31,)),
                pltpu.SemaphoreType.DMA((13,)),
                pltpu.SemaphoreType.DMA((13,)),
                pltpu.SemaphoreType.REGULAR,
                pltpu.SemaphoreType.REGULAR((7,)),
            ],
            compiler_params=pltpu.CompilerParams(
                collective_id=0, has_side_effects=True, vmem_limit_bytes=38 * 2**20),
            name="mlp_step",
        )(*args)
        dx_t, gn, dw = pl.pallas_call(
            second,
            in_specs=[vmem] * len(parts),
            out_specs=[hbm] * 3,
            out_shape=[jax.ShapeDtypeStruct(shape, dtype) for shape, dtype in
                       (((micro, d_model, tokens), BF16), ((3, blk, d_model), F32), ((3, d_model, ff), F32))],
            scratch_shapes=[pltpu.VMEM((3, d_model, ff), F32), pltpu.SemaphoreType.DMA((6,))],
            compiler_params=pltpu.CompilerParams(vmem_limit_bytes=12 * 2**20),
            name="second",
        )(*parts)
        return dx_t.transpose(0, 2, 1), gn.transpose(0, 2, 1), dw[None]

    in_specs = (P(None, TOK_AXES, None), P(None, TOK_AXES, None), P(None, GROUP_AXES), P(None, GROUP_AXES), P(GROUP_AXES, None), P(TOK_AXES, None, None, None))
    out_specs = (P(None, TOK_AXES, None), P(None, None, GROUP_AXES), P(TOK_AXES, None, None, None))
    return jax.shard_map(local_step, mesh=mesh, in_specs=in_specs, out_specs=out_specs, check_vma=False)
```
